32 devices in a mesh: ep: 16 (over z, y, core), dp: 2 (over x).
Axes of the slice: x: 2, y: 2, z: 4, core: 2. Of those that a mesh axis runs over, the one named last changes fastest.
Arguments:
- tokens: bfloat16 [512, 3584], P(('ep', 'dp')), may hold values from -6 to 6
- norm_gain: float32 [3584], replicated, may hold values from 0.25 to 1.75
- router: bfloat16 [3584, 16], replicated, may hold values from -0.09375 to 0.09375
- next_router: bfloat16 [3584, 16], P('dp'), may hold values from -0.09375 to 0.09375
- expert_ids: int32 [512, 8], P(('ep', 'dp')), may hold values from 0 to 15, all different within a row; in each aligned block of 16 rows (0 to 15, 16 to 31, ...) at most 16 rows name the same one
- store: bfloat16 [16, 2, 224, 128, 128], P('ep', 'dp'), may hold values from -0.125 to 0.125
- send_list: int32 [16, 224], P('ep'), may hold values from -1 to 223, as said below
- cache_map: int32 [16, 224], P('ep'), may hold values from 0 to 223, as said below
Outputs:
- layer_out: bfloat16 [512, 3584], P(('ep', 'dp'))
- next_scores: float32 [512, 16], P(('ep', 'dp'))
The draws below stay inside these ranges and needn't reach their ends.
Inputs may be any that keep to these rules, and one draw needn't show every extreme that they name: `expert_ids`: each row names 8 different experts; among the rows of one device no expert is named by more than 16 rows, a bound that some block reaches. `send_list`: an entry is -1 where that arriving slot stays empty; every row names each of the 224 store indices exactly once. `cache_map`: each entry numbers an arriving slot of that device that is never empty; the entries of a row are distinct.
All inputs are finite; a program needn't handle non-finite values.
Results may differ from the reference program's by a relative error of at most 0.0095.
Values may be sent and summed in bfloat16 or wider, within the bound.
No kernel may reach another device: no remote copies, remote signals or barrier semaphores. Data moves between devices by JAX's collectives and lax.ppermute only.
A program may use at most 64 MiB of HBM per device.

```python
import math
import jax
import jax.numpy as jnp
import numpy as np
from jax import lax

D = 3584
FF = 1024
TOP = 8
TR = 128
TC = 128
TOK_DEV = 16
EXPERTS = 16
CAP = 16
TILES_DEV = 224
PB = 14
TOKENS = 512
N_EP = 16
N_DP = 2


def tile_layout(key):
    count = N_EP * PB
    key_pairs, key_order, key_local = jax.random.split(jax.random.fold_in(key, 7), 3)
    pairs = jax.random.permutation(key_pairs, count)[:TILES_DEV]
    offsets = pairs // PB
    lanes = pairs % PB
    order = jax.random.permutation(key_order, N_EP)
    position = jnp.argsort(order)
    owner = order[(position[:, None] + offsets[None, :]) % N_EP]
    local_keys = jax.random.split(key_local, N_EP)
    local = jax.vmap(lambda single: jax.random.permutation(single, TILES_DEV))(local_keys)
    devices = jnp.arange(N_EP, dtype=jnp.int32)[:, None] + jnp.zeros((1, TILES_DEV), jnp.int32)
    columns = devices * PB + lanes[None, :]
    chosen = local[owner, jnp.arange(TILES_DEV, dtype=jnp.int32)[None, :]]
    listing = jnp.full((N_EP, count), -1, jnp.int32)
    listing = listing.at[owner.reshape(-1), columns.reshape(-1)].set(chosen.reshape(-1).astype(jnp.int32))
    mapping = (owner * PB + lanes[None, :]).astype(jnp.int32)
    return (listing, mapping)


def draw_send_list(key, part):
    return tile_layout(key)[0]


def draw_cache_map(key, part):
    return tile_layout(key)[1]


def levels(rng, shape, cuts, least, largest):
    def one(dim, shards_of):
        draws = jax.random.uniform(jax.random.fold_in(jax.random.fold_in(rng, 6), dim), (shards_of,), jnp.float32, least / len(cuts), largest / len(cuts))
        return jnp.repeat(jnp.exp(draws), shape[dim] // shards_of).reshape((-1,) + (1,) * (len(shape) - dim - 1))

    level = one(*cuts[0])
    for cut in cuts[1:]:
        level = level * one(*cut)
    return level


def routed_block(own_key, own, number, rows, count, top, most, lean):
    sequence = jax.random.permutation(own_key, count)
    packed, common = portions_of(count, rows * top, most, lean, True), portions_of(count, rows * top, most, lean, False)
    places = jnp.arange(count)

    def named(sizes, rotation):
        used = int((sizes > 0).sum())
        fixed = max(1, used // 4)
        shifted = fixed + (places - fixed + rotation * (used - fixed)) % max(1, count - fixed)
        return jnp.zeros((count,), jnp.int32).at[sequence[jnp.where(places < fixed, places, shifted)]].set(jnp.asarray(sizes, jnp.int32))

    sizes = jnp.where(number % 4 == 0, named(packed, number // 4), named(common, number - number // 4 - 1))
    mixed = jax.random.permutation(jax.random.fold_in(own, 3), count)
    source_of, taker = mixed[0:count // 2 * 2:2], mixed[1:count // 2 * 2:2]
    slack = jnp.minimum(sizes[source_of] - 1, most - sizes[taker]) // 2
    slack = jnp.where((source_of == sequence[0]) | (taker == sequence[0]) | (sizes[taker] == 0), 0, jnp.maximum(slack, 0))
    shifted = jax.random.randint(jax.random.fold_in(own, 4), (count // 2,), 0, 1 << 20) % (slack + 1)
    sizes = sizes.at[source_of].add(-shifted).at[taker].add(shifted)
    labels = jnp.searchsorted(jnp.cumsum(sizes), jnp.arange(rows * top), side="right").astype(jnp.int32)
    table = labels.reshape(top, rows).T
    table = table[jax.random.permutation(jax.random.fold_in(own, 1), rows)]
    rotation = jax.random.randint(jax.random.fold_in(own, 2), (rows, 1), 0, top)
    return jnp.take_along_axis(table, (jnp.arange(top)[None, :] + rotation) % top, axis=1)


def portions_of(amount, total, most, lean, full):
    portions = [(1 << 20) // math.isqrt(grade ** lean) + 1 for grade in range(1, amount + 1)]
    largest = most if full else min(most, max(-(-total // amount), total * portions[0] // sum(portions)))
    least = 1 if total - largest >= amount - 1 else 0
    holding, rest = [largest] + [least] * (amount - 1), total - largest - least * (amount - 1)
    while rest > 0:
        candidates = [i for i in range(1, amount) if holding[i] < largest] or [i for i in range(1, amount) if holding[i] < most]
        mass, remaining = sum([portions[i] for i in candidates]), rest
        for i in candidates:
            addition = min(most - holding[i], max(1, remaining * portions[i] // mass), rest)
            holding[i] = holding[i] + addition
            rest = rest - addition
    return np.array(holding)


def bell_draw(key, shape, scale, most, pieces=(), kind=jnp.bfloat16):
    drawn = scale * jax.random.normal(key, shape, jnp.float32)
    if pieces:
        drawn = drawn * levels(key, shape, pieces, -0.22, 0.18)
    return jnp.clip(drawn, -most, most).astype(kind)


def setup_inputs(seed: int = 0) -> dict:
    splits = jax.random.split(jax.random.key(seed), 9)
    tokens = bell_draw(splits[0], (TOKENS, D), 1.0, 6.0, ((0, 32),))
    norm_gain = jnp.clip(1.0 + 0.15 * jax.random.normal(splits[1], (D,), jnp.float32), 0.25, 1.75)
    router = bell_draw(splits[2], (D, EXPERTS), D ** -0.5, 0.09375)
    next_router = bell_draw(splits[3], (D, EXPERTS), D ** -0.5, 0.09375, ((0, 2),))
    expert_ids_keys = jax.random.split(jax.random.fold_in(splits[4], 1), TOKENS // TOK_DEV)
    expert_ids_turns = jax.random.permutation(jax.random.fold_in(splits[4], 3), TOKENS // TOK_DEV)
    expert_ids = jax.vmap(lambda own, number: routed_block(jax.random.fold_in(splits[4], 2), own, number, TOK_DEV, EXPERTS, TOP, CAP, 2))(expert_ids_keys, expert_ids_turns).reshape((TOKENS, TOP))
    store = bell_draw(splits[5], (N_EP, N_DP, TILES_DEV, TR, TC), (2 * FF) ** -0.5, 0.125, ((0, 16), (1, 2)))
    send_list = draw_send_list(jax.random.fold_in(splits[8], 71), 0)
    cache_map = draw_cache_map(jax.random.fold_in(splits[8], 71), 0)
    return dict(tokens=tokens, norm_gain=norm_gain, router=router, next_router=next_router, expert_ids=expert_ids, store=store, send_list=send_list, cache_map=cache_map)


def reference(tokens, norm_gain, router, next_router, expert_ids, store, send_list, cache_map):
    values = tokens.astype(jnp.float32)
    scale = lax.rsqrt(lax.optimization_barrier(jnp.mean(values * values, axis=1, keepdims=True)) + 1e-06)
    normed = (values * scale * norm_gain).astype(jnp.bfloat16)
    scores = jax.nn.sigmoid(jnp.dot(normed, router, preferred_element_type=jnp.float32))
    picked = jnp.take_along_axis(scores, expert_ids, axis=1)
    weights = (2.5 * picked / lax.optimization_barrier(jnp.sum(picked, axis=1, keepdims=True))).astype(jnp.bfloat16)
    count = tokens.shape[0]
    limit = N_DP * N_EP * CAP
    row_tiles = D // (N_DP * TR)
    col_tiles = FF // TC

    def one_expert(total, expert):
        mapping = cache_map[expert]
        owners = mapping // PB
        lanes = mapping % PB
        local = send_list[owners, expert * PB + lanes]
        blocks = []
        for group in range(N_DP):
            tiles = store[owners, group, jnp.maximum(local, 0)]
            tiles = jnp.where((local >= 0)[:, None, None], tiles, jnp.zeros((), jnp.bfloat16))
            blocks.append(tiles.reshape(2, row_tiles, col_tiles, TR, TC))
        stacked = jnp.stack(blocks, axis=1)
        weight = stacked.transpose(0, 1, 2, 4, 3, 5).reshape(2, D, FF)
        hit = expert_ids == expert
        routed = jnp.any(hit, axis=1)
        factor = lax.optimization_barrier(jnp.sum(jnp.where(hit, weights.astype(jnp.float32), jnp.float32(0.0)), axis=1))
        order = jnp.cumsum(routed.astype(jnp.int32)).astype(jnp.int32) - 1
        target = jnp.where(routed, order, limit).astype(jnp.int32)
        index = jnp.zeros((limit,), jnp.int32).at[target].set(jnp.arange(count, dtype=jnp.int32), mode='drop')
        valid = jnp.zeros((limit,), jnp.float32).at[target].set(jnp.float32(1.0), mode='drop')
        rows = normed[index]
        pre = jnp.dot(rows, weight[0], preferred_element_type=jnp.float32)
        hidden = jax.nn.silu(pre).astype(jnp.bfloat16)
        out = lax.dot_general(hidden, weight[1], (((1,), (1,)), ((), ())), preferred_element_type=jnp.float32).astype(jnp.bfloat16)
        term = out.astype(jnp.float32) * (factor[index] * valid)[:, None]
        return (total.at[index].add(term), None)
    total, _ = lax.scan(one_expert, values, jnp.arange(EXPERTS, dtype=jnp.int32))
    layer_out = total.astype(jnp.bfloat16)
    stream = layer_out.astype(jnp.float32)
    renorm = lax.rsqrt(lax.optimization_barrier(jnp.mean(stream * stream, axis=1, keepdims=True)) + 1e-06)
    next_normed = (stream * renorm).astype(jnp.bfloat16)
    next_scores = jax.nn.sigmoid(jnp.dot(next_normed, next_router, preferred_element_type=jnp.float32))
    return (layer_out, next_scores)
```

```python
import functools

import jax
import jax.numpy as jnp
from jax import lax
from jax.experimental import pallas as pl
from jax.experimental.pallas import tpu as pltpu
from jax.sharding import PartitionSpec as P

ANY = pl.BlockSpec(memory_space=pl.ANY)
VMEM = pl.BlockSpec(memory_space=pltpu.VMEM)
SMEM = pl.BlockSpec(memory_space=pltpu.SMEM)


def largest_divisor(number, most):
    return max(d for d in range(1, most + 1) if number % d == 0)


def pick_kernel(chunks, size, index_ref, store_ref, out_ref, held, in_sems, out_sem):
    for chunk in range(chunks):

        def fetch(i, carry, chunk=chunk):
            slot = chunk * size + i
            tile = jnp.maximum(index_ref[slot], 0)
            pltpu.make_async_copy(store_ref.at[tile], held.at[slot], in_sems.at[chunk]).start()
            return carry

        lax.fori_loop(0, size, fetch, 0)
    for chunk in range(chunks):
        block = pl.ds(chunk * size, size)
        pltpu.make_async_copy(held.at[block], held.at[block], in_sems.at[chunk]).wait()
        pltpu.make_async_copy(held.at[block], out_ref.at[block], out_sem).start()
    pltpu.make_async_copy(held, out_ref, out_sem).wait()


def pick_tiles(store, index):
    slots = index.shape[0]
    chunks = largest_divisor(slots, 8)
    shape = (slots,) + store.shape[1:]
    return pl.pallas_call(
        functools.partial(pick_kernel, chunks, slots // chunks),
        out_shape=jax.ShapeDtypeStruct(shape, store.dtype),
        in_specs=[SMEM, ANY],
        out_specs=ANY,
        scratch_shapes=[
            pltpu.VMEM(shape, store.dtype),
            pltpu.SemaphoreType.DMA((chunks,)),
            pltpu.SemaphoreType.DMA,
        ],
        name="pick_tiles",
    )(index, store)


def up_kernel(step, map_ref, rows_ref, tiles_ref, out_ref, weight, sems):
    tile_rows, tile_cols = tiles_ref.shape[1:]
    part, width = weight.shape
    row_tiles, col_tiles = part // tile_rows, width // tile_cols
    blocks = col_tiles // step

    def fetch(i, carry):
        for column in range(col_tiles):
            slot = map_ref[i * col_tiles + column]
            start = pl.multiple_of(i * tile_rows, tile_rows)
            pltpu.make_async_copy(
                tiles_ref.at[slot],
                weight.at[pl.ds(start, tile_rows), pl.ds(column * tile_cols, tile_cols)],
                sems.at[column // step],
            ).start()
        return carry

    lax.fori_loop(0, row_tiles, fetch, 0)
    rows = rows_ref[:, :part]
    for block in range(blocks):
        columns = pl.ds(block * step * tile_cols, step * tile_cols)
        piece = weight.at[:, columns]
        pltpu.make_async_copy(piece, piece, sems.at[block]).wait()
        out_ref[:, columns] = jnp.dot(
            rows, piece[...], preferred_element_type=jnp.float32
        ).astype(out_ref.dtype)


def up_product(index, rows, tiles, part, width):
    step = largest_divisor(width // tiles.shape[2], 2)
    blocks = width // tiles.shape[2] // step
    count = rows.shape[0]
    return pl.pallas_call(
        functools.partial(up_kernel, step),
        out_shape=jax.ShapeDtypeStruct((count, width), jnp.bfloat16),
        in_specs=[SMEM, VMEM, ANY],
        out_specs=VMEM,
        scratch_shapes=[
            pltpu.VMEM((part, width), tiles.dtype),
            pltpu.SemaphoreType.DMA((blocks,)),
        ],
        cost_estimate=pl.CostEstimate(
            flops=2 * count * part * width,
            bytes_accessed=2 * (part * width + count * (part + width)),
            transcendentals=0,
        ),
        name="up_product",
    )(index, rows, tiles)


def down_kernel(step, first, map_ref, factor_ref, own_ref, other_ref, tiles_ref, out_ref, weight, hidden, sems):
    tile_rows, tile_cols = tiles_ref.shape[1:]
    part, width = weight.shape
    row_tiles, col_tiles = part // tile_rows, width // tile_cols
    blocks = row_tiles // step
    half = own_ref.shape[0] // 2
    for block in range(blocks):

        def fetch(i, carry, block=block):
            row = block * step + i
            for column in range(col_tiles):
                slot = map_ref[first + row * col_tiles + column]
                start = pl.multiple_of(row * tile_rows, tile_rows)
                pltpu.make_async_copy(
                    tiles_ref.at[slot],
                    weight.at[pl.ds(start, tile_rows), pl.ds(column * tile_cols, tile_cols)],
                    sems.at[block],
                ).start()
            return carry

        lax.fori_loop(0, step, fetch, 0)
    for side in range(2):
        mine, theirs = pl.ds(side * half, half), pl.ds((1 - side) * half, half)
        pre = own_ref[mine, :].astype(jnp.float32) + other_ref[theirs, :].astype(jnp.float32)
        hidden[mine, :] = (pre * jax.nn.sigmoid(pre)).astype(hidden.dtype)
    units = hidden[...]
    factor = factor_ref[...]
    for block in range(blocks):
        piece = weight.at[pl.ds(block * step * tile_rows, step * tile_rows), :]
        pltpu.make_async_copy(piece, piece, sems.at[block]).wait()
        product = lax.dot_general(
            units, piece[...], (((1,), (1,)), ((), ())), preferred_element_type=jnp.float32
        )
        out_ref[:, pl.ds(block * step * tile_rows, step * tile_rows)] = (
            product * factor
        ).astype(out_ref.dtype)


def down_product(index, first, factor, own, other, tiles, part):
    step = largest_divisor(part // tiles.shape[1], 2)
    blocks = part // tiles.shape[1] // step
    count, width = own.shape
    return pl.pallas_call(
        functools.partial(down_kernel, step, first),
        out_shape=jax.ShapeDtypeStruct((count, part), jnp.bfloat16),
        in_specs=[SMEM, VMEM, VMEM, VMEM, ANY],
        out_specs=VMEM,
        scratch_shapes=[
            pltpu.VMEM((part, width), tiles.dtype),
            pltpu.VMEM((count, width), jnp.bfloat16),
            pltpu.SemaphoreType.DMA((blocks,)),
        ],
        cost_estimate=pl.CostEstimate(
            flops=2 * count * part * width,
            bytes_accessed=2 * (part * width + count * (part + 2 * width)),
            transcendentals=count * width,
        ),
        name="down_product",
    )(index, factor, own, other, tiles)


def flip(value, axis, bit):
    return lax.ppermute(value, axis, [(i, i ^ bit) for i in range(lax.axis_size(axis))])


def dense_layer(tokens, norm_gain, router, next_router, expert_ids, store, send_list, cache_map):
    tok_dev, width = tokens.shape
    n_ep = lax.axis_size("ep")
    experts = router.shape[1]
    tiles = cache_map.shape[1]
    tile_rows, tile_cols = store.shape[3:]
    part = width // 2
    row_tiles = part // tile_rows
    col_tiles = tiles // (2 * row_tiles)
    hidden_width = col_tiles * tile_cols
    me, side = lax.axis_index("ep"), lax.axis_index("dp")

    leaving = pick_tiles(store.reshape(tiles, tile_rows, tile_cols), send_list.reshape(-1))
    arrived = lax.all_to_all(leaving, "ep", split_axis=0, concat_axis=0, tiled=True)

    values = tokens.astype(jnp.float32)
    scale = lax.rsqrt(jnp.mean(values * values, axis=1, keepdims=True) + 1e-06)
    normed = (values * scale * norm_gain).astype(jnp.bfloat16)
    scores = jax.nn.sigmoid(jnp.dot(normed, router, preferred_element_type=jnp.float32))
    chosen = (
        expert_ids[:, :, None] == jnp.arange(experts, dtype=jnp.int32)[None, None, :]
    ).astype(jnp.float32)
    named = jnp.sum(chosen, axis=1)
    picked = named * scores
    weights = (2.5 * picked / jnp.sum(picked, axis=1, keepdims=True)).astype(jnp.bfloat16)
    lanes = tile_cols * (-(-experts // tile_cols))
    weights = jnp.pad(weights, ((0, 0), (0, lanes - experts)))
    first, second = normed[:, :part], normed[:, part:]
    mine = jnp.concatenate([jnp.where(side == 0, first, second), weights], axis=1)
    theirs = jnp.concatenate([jnp.where(side == 0, second, first), weights], axis=1)
    rows, other_router = lax.optimization_barrier(
        (jnp.stack([mine, flip(theirs, "dp", 1)]), flip(next_router, "dp", 1))
    )
    far = n_ep // 2
    bits = [far]
    while far > 1:
        far //= 2
        bits.append(far)
    for bit in bits:
        rows = jnp.concatenate([rows, flip(rows, "ep", bit)], axis=1)
    rows = rows.reshape(2 * n_ep * tok_dev, part + lanes)
    lane = lax.broadcasted_iota(jnp.int32, (1, lanes), 1)
    factor = jnp.sum(
        jnp.where(lane == me, rows[:, part:].astype(jnp.float32), 0.0), axis=1, keepdims=True
    )
    index = cache_map.reshape(-1)
    pre = up_product(index, rows, arrived, part, hidden_width)
    product = down_product(
        index, row_tiles * col_tiles, factor, pre, flip(pre, "dp", 1), arrived, part
    )
    total = product.reshape(2, n_ep * tok_dev, part)
    for bit in bits[::-1]:
        count = total.shape[1] // 2
        got = flip(total[:, count:], "ep", bit)
        total = total[:, :count].astype(jnp.float32) + got.astype(jnp.float32)
        if bit != bits[0]:
            total = total.astype(jnp.bfloat16)
    total = total.astype(jnp.bfloat16)
    other = flip(total[1], "dp", 1)
    mine = total[0]
    mixed = jnp.where(
        side == 0,
        jnp.concatenate([mine, other], axis=1),
        jnp.concatenate([other, mine], axis=1),
    ).astype(jnp.float32)
    layer_out = (values + mixed).astype(jnp.bfloat16)
    stream = layer_out.astype(jnp.float32)
    renorm = lax.rsqrt(jnp.mean(stream * stream, axis=1, keepdims=True) + 1e-06)
    next_normed = (stream * renorm).astype(jnp.bfloat16)
    whole_router = jnp.where(
        side == 0,
        jnp.concatenate([next_router, other_router], axis=0),
        jnp.concatenate([other_router, next_router], axis=0),
    )
    next_logits = jnp.dot(next_normed, whole_router, preferred_element_type=jnp.float32)
    return (layer_out, jax.nn.sigmoid(next_logits))


def sparse_layer(tokens, norm_gain, router, next_router, expert_ids, store, send_list, cache_map):
    tok_dev, width = tokens.shape
    n_dp = lax.axis_size("dp")
    experts = router.shape[1]
    top = expert_ids.shape[1]
    tiles = cache_map.shape[1]
    tile_rows = store.shape[3]
    tile_cols = store.shape[4]
    part = width // n_dp
    row_tiles = part // tile_rows
    col_tiles = tiles // (2 * row_tiles)
    hidden_width = col_tiles * tile_cols
    capacity = row_capacity(tokens, router, expert_ids)
    values = tokens.astype(jnp.float32)
    scale = lax.rsqrt(jnp.mean(values * values, axis=1, keepdims=True) + 1e-06)
    normed = (values * scale * norm_gain).astype(jnp.bfloat16)
    scores = jax.nn.sigmoid(jnp.dot(normed, router, preferred_element_type=jnp.float32))
    chosen = (expert_ids[:, :, None] == jnp.arange(experts, dtype=jnp.int32)[None, None, :]).astype(
        jnp.float32
    )
    picked = jnp.sum(chosen * scores[:, None, :], axis=2)
    weights = (2.5 * picked / jnp.sum(picked, axis=1, keepdims=True)).astype(jnp.bfloat16)
    flat = chosen.reshape(tok_dev * top, experts)
    before = jnp.cumsum(flat, axis=0) - flat
    rank = jnp.sum(before * flat, axis=1).astype(jnp.int32)
    slot = expert_ids.reshape(-1) * capacity + rank
    columns = jnp.arange(experts * capacity, dtype=jnp.int32)
    match = (slot[:, None] == columns[None, :]).reshape(tok_dev, top, experts * capacity)
    dispatch = jnp.sum(match.astype(jnp.float32), axis=1).astype(jnp.bfloat16)
    combine = jnp.sum(
        jnp.where(match, weights.astype(jnp.float32)[:, :, None], 0.0), axis=1
    ).astype(jnp.bfloat16)
    outgoing = lax.dot_general(
        dispatch, normed, (((0,), (0,)), ((), ())), preferred_element_type=jnp.float32
    ).astype(jnp.bfloat16)
    owned = store.reshape(store.shape[2], tile_rows, tile_cols)
    leaving = owned[jnp.maximum(send_list.reshape(-1), 0)]
    arrived = lax.all_to_all(leaving, "ep", split_axis=0, concat_axis=0, tiled=True)
    cached = arrived[cache_map.reshape(-1)].reshape(2, row_tiles, col_tiles, tile_rows, tile_cols)
    up_tiles = cached[0]
    down_tiles = cached[1]
    rows = lax.all_to_all(
        lax.all_to_all(outgoing, "ep", split_axis=0, concat_axis=0, tiled=True),
        "dp",
        split_axis=1,
        concat_axis=0,
        tiled=True,
    )
    count = rows.shape[0]
    block = rows.reshape(count, row_tiles, tile_rows)
    product = jnp.einsum("nat,acts->ncs", block, up_tiles, preferred_element_type=jnp.float32)
    summed = lax.psum(product.reshape(count, hidden_width).astype(jnp.bfloat16), "dp").astype(
        jnp.float32
    )
    hidden = jax.nn.silu(summed).astype(jnp.bfloat16)
    number = hidden.shape[0]
    product = jnp.einsum(
        "ncs,acts->nat",
        hidden.reshape(number, col_tiles, tile_cols),
        down_tiles,
        preferred_element_type=jnp.float32,
    )
    result = product.reshape(number, part).astype(jnp.bfloat16)
    back = lax.all_to_all(
        lax.all_to_all(result, "dp", split_axis=0, concat_axis=1, tiled=True),
        "ep",
        split_axis=0,
        concat_axis=0,
        tiled=True,
    )
    mixed = jnp.dot(combine, back, preferred_element_type=jnp.float32)
    layer_out = (values + mixed).astype(jnp.bfloat16)
    stream = layer_out.astype(jnp.float32)
    renorm = lax.rsqrt(jnp.mean(stream * stream, axis=1, keepdims=True) + 1e-06)
    next_normed = (stream * renorm).astype(jnp.bfloat16)
    features = lax.all_to_all(next_normed, "dp", split_axis=1, concat_axis=0, tiled=True)
    partial_scores = jnp.dot(features, next_router, preferred_element_type=jnp.float32)
    next_logits = lax.psum_scatter(
        partial_scores.astype(jnp.bfloat16), "dp", scatter_dimension=0, tiled=True
    ).astype(jnp.float32)
    return (layer_out, jax.nn.sigmoid(next_logits))


def row_capacity(tokens, router, expert_ids):
    tok_dev, experts, top = tokens.shape[0], router.shape[1], expert_ids.shape[1]
    return min(tok_dev, max(2, 2 * tok_dev * top // experts))


def per_device(*arrays):
    tokens, _, router, _, expert_ids, store, _, cache_map = arrays
    n_ep = lax.axis_size("ep")
    every_row = row_capacity(tokens, router, expert_ids) == tokens.shape[0]
    one_each = router.shape[1] == n_ep and store.shape[2] == cache_map.shape[1]
    if every_row and one_each and lax.axis_size("dp") == 2 and n_ep & (n_ep - 1) == 0:
        return dense_layer(*arrays)
    return sparse_layer(*arrays)


def solution(mesh):
    in_specs = (
        P(("ep", "dp"), None),
        P(),
        P(),
        P("dp", None),
        P(("ep", "dp"), None),
        P("ep", "dp", None, None, None),
        P("ep", None),
        P("ep", None),
    )
    out_specs = (P(("ep", "dp"), None), P(("ep", "dp"), None))
    return jax.shard_map(
        per_device, mesh=mesh, in_specs=in_specs, out_specs=out_specs, check_vma=False
    )
```

```python
import functools

import jax
import jax.numpy as jnp
from jax import lax
from jax.experimental import pallas as pl
from jax.experimental.pallas import tpu as pltpu
from jax.sharding import PartitionSpec as P


ANY = pl.BlockSpec(memory_space=pl.ANY)
VMEM = pl.BlockSpec(memory_space=pltpu.VMEM)
SMEM = pl.BlockSpec(memory_space=pltpu.SMEM)


def largest_divisor(number, most):
    return max(d for d in range(1, most + 1) if number % d == 0)


def pick_kernel(column_of, chunks, size, place_ref, list_ref, store_ref, *refs):
    outs, (held, in_sems, out_sem) = refs[:-3], refs[-3:]
    place = place_ref[0]
    for chunk in range(chunks):

        def fetch(i, carry, chunk=chunk):
            tile = list_ref[column_of(place, chunk, i)]
            copy = pltpu.make_async_copy(
                store_ref.at[tile], held.at[chunk * size + i], in_sems.at[chunk]
            )
            copy.start()
            return carry

        lax.fori_loop(0, size, fetch, 0)
    puts = []
    for chunk in range(chunks):
        block = held.at[pl.ds(chunk * size, size)]
        pltpu.make_async_copy(block, block, in_sems.at[chunk]).wait()
        target = outs[chunk] if len(outs) > 1 else outs[0].at[pl.ds(chunk * size, size)]
        puts.append(pltpu.make_async_copy(block, target, out_sem.at[chunk]))
        puts[-1].start()
    for put in puts:
        put.wait()


def pick_tiles(column_of, place, wanted, store, chunks, size, joined):
    tile = store.shape[1:]
    if joined:
        shapes = jax.ShapeDtypeStruct((chunks * size,) + tile, store.dtype)
    else:
        shapes = [jax.ShapeDtypeStruct((size,) + tile, store.dtype)] * chunks
    return pl.pallas_call(
        functools.partial(pick_kernel, column_of, chunks, size),
        out_shape=shapes,
        in_specs=[SMEM, SMEM, ANY],
        out_specs=ANY if joined else [ANY] * chunks,
        scratch_shapes=[
            pltpu.VMEM((chunks * size,) + tile, store.dtype),
            pltpu.SemaphoreType.DMA((chunks,)),
            pltpu.SemaphoreType.DMA((chunks,)),
        ],
        cost_estimate=pl.CostEstimate(
            flops=chunks * size * 2**24, bytes_accessed=chunks * size * 2**17, transcendentals=0
        ),
    )(place, wanted, store)


def scatter_tiles(first, map_ref, tile_refs, sources, weight, sem_of):
    tile_rows, tile_cols = sources[0].shape[1:]
    part, width = weight.shape
    row_tiles, col_tiles = part // tile_rows, width // tile_cols

    def place_of(s):
        row, column = lax.div(s, col_tiles), lax.rem(s, col_tiles)
        rows = pl.ds(pl.multiple_of(row * tile_rows, tile_rows), tile_rows)
        columns = pl.ds(pl.multiple_of(column * tile_cols, tile_cols), tile_cols)
        return row, column, weight.at[rows, columns]

    begin = 0
    for source in sources:

        def fetch(i, carry, source=source, begin=begin):
            s = tile_refs[begin + i] - first

            @pl.when((s >= 0) & (s < row_tiles * col_tiles))
            def _():
                row, column, place = place_of(s)
                pltpu.make_async_copy(source.at[i], place, sem_of(row, column)).start()

            return carry

        lax.fori_loop(0, source.shape[0], fetch, 0, unroll=source.shape[0] < 8)
        begin += source.shape[0]

    def clear(row, carry):
        for column in range(col_tiles):

            @pl.when(map_ref[first + row * col_tiles + column] < 0)
            def _(column=column):
                rows = pl.ds(pl.multiple_of(row * tile_rows, tile_rows), tile_rows)
                weight[rows, pl.ds(column * tile_cols, tile_cols)] = jnp.zeros(
                    (tile_rows, tile_cols), weight.dtype
                )

        return carry

    lax.fori_loop(0, row_tiles, clear, 0)


def wait_tiles(first, map_ref, weight, tile, sem, rows, columns):
    tile_rows, tile_cols = tile
    col_tiles = weight.shape[1] // tile_cols

    def wait(i, carry):
        row = rows[0] + i
        for column in columns:

            @pl.when(map_ref[first + row * col_tiles + column] >= 0)
            def _(column=column):
                place = weight.at[
                    pl.ds(pl.multiple_of(row * tile_rows, tile_rows), tile_rows),
                    pl.ds(column * tile_cols, tile_cols),
                ]
                pltpu.make_async_copy(place, place, sem).wait()

        return carry

    lax.fori_loop(0, rows[1], wait, 0)


def up_kernel(step, map_ref, tile_refs, rows_ref, *refs):
    sources, (out_ref, weight, sems) = refs[:-3], refs[-3:]
    tile = sources[0].shape[1:]
    part, width = weight.shape
    row_tiles, col_tiles = part // tile[0], width // tile[1]
    scatter_tiles(
        0, map_ref, tile_refs, sources, weight, lambda row, column: sems.at[lax.div(column, step)]
    )
    rows = rows_ref[:, :part]
    for block in range(col_tiles // step):
        wait_tiles(
            0,
            map_ref,
            weight,
            tile,
            sems.at[block],
            (0, row_tiles),
            range(block * step, block * step + step),
        )
        columns = pl.ds(block * step * tile[1], step * tile[1])
        out_ref[:, columns] = jnp.dot(
            rows, weight[:, columns], preferred_element_type=jnp.float32
        ).astype(out_ref.dtype)


def up_product(index, inverse, rows, sources, part, width):
    tile_cols = sources[0].shape[2]
    step = largest_divisor(width // tile_cols, 4)
    count = rows.shape[0]
    return pl.pallas_call(
        functools.partial(up_kernel, step),
        out_shape=jax.ShapeDtypeStruct((count, width), jnp.bfloat16),
        in_specs=[SMEM, SMEM, VMEM] + [ANY] * len(sources),
        out_specs=VMEM,
        scratch_shapes=[
            pltpu.VMEM((part, width), sources[0].dtype),
            pltpu.SemaphoreType.DMA((width // tile_cols // step,)),
        ],
        cost_estimate=pl.CostEstimate(
            flops=2 * count * part * width,
            bytes_accessed=2 * (part * width + count * (part + width)),
            transcendentals=0,
        ),
        name="up_product",
    )(index, inverse, rows, *sources)


def place_kernel(first, chunks, map_ref, tile_refs, *refs):
    sources, (out_ref, weight, in_sems, out_sems) = refs[:-4], refs[-4:]
    tile = sources[0].shape[1:]
    part, width = weight.shape
    size = part // tile[0] // chunks
    scatter_tiles(
        first, map_ref, tile_refs, sources, weight, lambda row, column: in_sems.at[lax.div(row, size)]
    )
    puts = []
    for chunk in range(chunks):
        wait_tiles(
            first,
            map_ref,
            weight,
            tile,
            in_sems.at[chunk],
            (chunk * size, size),
            range(width // tile[1]),
        )
        block = pl.ds(chunk * size * tile[0], size * tile[0])
        puts.append(pltpu.make_async_copy(weight.at[block], out_ref.at[block], out_sems.at[chunk]))
        puts[-1].start()
    for put in puts:
        put.wait()


def place_down(index, inverse, first, sources, part, width):
    chunks = largest_divisor(part // sources[0].shape[1], 4)
    return pl.pallas_call(
        functools.partial(place_kernel, first, chunks),
        out_shape=jax.ShapeDtypeStruct((part, width), sources[0].dtype),
        in_specs=[SMEM, SMEM] + [ANY] * len(sources),
        out_specs=ANY,
        scratch_shapes=[
            pltpu.VMEM((part, width), sources[0].dtype),
            pltpu.SemaphoreType.DMA((chunks,)),
            pltpu.SemaphoreType.DMA((chunks,)),
        ],
        cost_estimate=pl.CostEstimate(
            flops=part * width * 1024, bytes_accessed=4 * part * width, transcendentals=0
        ),
        name="place_down",
    )(index, inverse, *sources)


def down_kernel(*refs):
    experts = len(refs) // 3
    out_ref = refs[-1]
    total = 0.0
    for e in range(experts):
        weight, units, factor = refs[3 * e : 3 * e + 3]
        product = lax.dot_general(
            units[...], weight[...], (((1,), (1,)), ((), ())), preferred_element_type=jnp.float32
        )
        total = total + product * factor[...]
    out_ref[...] = total.astype(out_ref.dtype)


def down_product(weights, units, factors, block):
    part, width = weights[0].shape
    count = units[0].shape[0]
    specs, operands = [], []
    for weight, unit, factor in zip(weights, units, factors, strict=True):
        specs += [
            pl.BlockSpec((block, width), lambda i: (i, 0)),
            pl.BlockSpec((count, width), lambda i: (0, 0)),
            pl.BlockSpec((count, 1), lambda i: (0, 0)),
        ]
        operands += [weight, unit, factor]
    return pl.pallas_call(
        down_kernel,
        grid=(part // block,),
        out_shape=jax.ShapeDtypeStruct((count, part), jnp.bfloat16),
        in_specs=specs,
        out_specs=pl.BlockSpec((count, block), lambda i: (0, i)),
        cost_estimate=pl.CostEstimate(
            flops=2 * len(weights) * count * part * width,
            bytes_accessed=2 * (len(weights) * (part + count) * width + count * part),
            transcendentals=0,
        ),
        name="down_product",
    )(*operands)


def flip(value, axis, bit):
    return lax.ppermute(value, axis, [(i, i ^ bit) for i in range(lax.axis_size(axis))])


def silu_sum(first, second):
    pre = first.astype(jnp.float32) + second.astype(jnp.float32)
    return (pre * jax.nn.sigmoid(pre)).astype(jnp.bfloat16)


def plain_sum(first, second):
    return (first.astype(jnp.float32) + second.astype(jnp.float32)).astype(jnp.bfloat16)


def take(value, axis, which):
    return lax.index_in_dim(value, which, axis, keepdims=True)


def add_up(value, steps):
    for combine, (axis, name, bit) in steps:
        value = combine(take(value, axis, 0), flip(take(value, axis, 1), name, bit))
    return value


def gather_back(value, steps):
    for axis, name, bit in steps:
        value = jnp.concatenate([value, flip(value, name, bit)], axis=axis)
    return value


def dense_layer(tokens, norm_gain, router, next_router, expert_ids, store, send_list, cache_map):
    tok_dev, width = tokens.shape
    n_ep = lax.axis_size("ep")
    half = n_ep // 2
    experts = router.shape[1]
    tiles = cache_map.shape[1]
    lanes_of = tiles // n_ep
    sub = lanes_of // 2
    tile_rows, tile_cols = store.shape[3:]
    part = width // 2
    row_tiles = part // tile_rows
    col_tiles = tiles // (2 * row_tiles)
    hidden_width = col_tiles * tile_cols
    me, side = lax.axis_index("ep"), lax.axis_index("dp")
    groups = [list(range(half)), list(range(half, n_ep))]
    mirror = ("ep", half)
    beside = ("ep", 1)
    across = ("dp", 1)

    owned = store.reshape(tiles, tile_rows, tile_cols)
    wanted = send_list.reshape(-1)
    place = jnp.reshape(me, (1,)).astype(jnp.int32)

    def near_column(number, i, lane):
        return i * lanes_of + lane

    def far_column(number, j, lane):
        return half * lanes_of + sub * (number ^ j) + lane

    leaving = pick_tiles(near_column, place, wanted, owned, half, lanes_of, True)
    far = pick_tiles(far_column, place, wanted, owned, n_ep, sub, False)

    values = tokens.astype(jnp.float32)
    scale = lax.rsqrt(jnp.mean(values * values, axis=1, keepdims=True) + 1e-06)
    normed = (values * scale * norm_gain).astype(jnp.bfloat16)
    scores = jax.nn.sigmoid(jnp.dot(normed, router, preferred_element_type=jnp.float32))
    chosen = (
        expert_ids[:, :, None] == jnp.arange(experts, dtype=jnp.int32)[None, None, :]
    ).astype(jnp.float32)
    picked = jnp.sum(chosen, axis=1) * scores
    weights = (2.5 * picked / jnp.sum(picked, axis=1, keepdims=True)).astype(jnp.bfloat16)
    digit = tile_cols
    each = -(-tiles // tok_dev)
    codes = jnp.pad(cache_map.reshape(-1), (0, each * tok_dev - tiles)).reshape(tok_dev, each)
    codes = jnp.concatenate([codes // digit, codes % digit], axis=1).astype(jnp.bfloat16)
    used = experts + 2 * each
    lanes = tile_cols * (-(-used // tile_cols))
    first, second = normed[:, :part], normed[:, part:]
    mine = jnp.concatenate(
        [
            jnp.where(side == 0, first, second),
            jnp.pad(jnp.concatenate([weights, codes], axis=1), ((0, 0), (0, lanes - used))),
        ],
        axis=1,
    )
    theirs = jnp.concatenate(
        [
            jnp.where(side == 0, second, first),
            jnp.pad(weights, ((0, 0), (0, lanes - experts))),
        ],
        axis=1,
    )
    rows, leaving = lax.optimization_barrier((jnp.stack([mine, flip(theirs, *across)]), leaving))
    arrived = lax.all_to_all(
        leaving, "ep", split_axis=0, concat_axis=0, tiled=True, axis_index_groups=groups
    )
    rows = jnp.stack([rows, flip(rows, *mirror)], axis=1)
    blocks = [rows]
    for number in range(2, half, 2):
        blocks.append(flip(rows, "ep", number))
    crossed = [far[0]]
    for j in range(1, n_ep):
        crossed.append(flip(far[j], "ep", j))
    rows = jnp.stack(blocks, axis=2)
    rows = jnp.stack([rows, flip(rows, *beside)], axis=2)
    rows = rows.reshape(2 * n_ep * tok_dev, part + lanes)
    rows, other_router = lax.optimization_barrier((rows, flip(next_router, *across)))

    def map_of(number):
        relative = number ^ me
        block = (relative // half * 2 + relative % 2) * (half // 2) + relative % half // 2
        got = lax.dynamic_slice(
            rows, (block * tok_dev, part + experts), (tok_dev, 2 * each)
        ).astype(jnp.int32)
        return (got[:, :each] * digit + got[:, each:]).reshape(-1)[:tiles]

    lane = lax.broadcasted_iota(jnp.int32, (1, lanes), 1)
    gates = rows[:, part:].astype(jnp.float32)
    expert_of = [me % half, half + me // 2]
    factors = [
        jnp.sum(jnp.where(lane == e, gates, 0.0), axis=1, keepdims=True) for e in expert_of
    ]

    slots = map_of(expert_of[0])
    owner, number = slots // lanes_of, slots % lanes_of
    near = (owner // half) == (me // half)
    map_a = jnp.where(near, owner % half * lanes_of + number, -1)
    slots = map_of(expert_of[1])
    owner, inside = slots // lanes_of, slots % lanes_of - sub * (me % 2)
    map_b = jnp.where((inside >= 0) & (inside < sub), (owner ^ me) * sub + inside, -1)

    def inverse_of(index):
        held = index[None, :] == jnp.arange(tiles // 2, dtype=jnp.int32)[:, None]
        number = jnp.arange(1, tiles + 1, dtype=jnp.int32)[None, :]
        return jnp.sum(jnp.where(held, number, 0), axis=1) - 1

    shape = (2, 2, 2, half // 2 * tok_dev, hidden_width)
    held_a = (map_a, inverse_of(map_a))
    held_b = (map_b, inverse_of(map_b))
    (map_a, inverse_a), (map_b, inverse_b) = lax.optimization_barrier((held_a, held_b))
    pre = up_product(map_a, inverse_a, rows, [arrived], part, hidden_width).reshape(shape)
    own = add_up(pre, [(plain_sum, (0,) + across)])
    down_a = place_down(map_a, inverse_a, tiles // 2, [arrived], part, hidden_width)
    own = silu_sum(take(own, 1, 0), flip(take(own, 1, 1), *mirror))
    kept, crossed, down_a = lax.optimization_barrier((own, crossed, down_a))
    units_a = jnp.concatenate([kept, flip(own, *mirror)], axis=1)
    units_a = gather_back(units_a, [(0,) + across])
    pre = up_product(map_b, inverse_b, rows, crossed, part, hidden_width).reshape(shape)
    own = add_up(pre, [(plain_sum, (2,) + beside), (silu_sum, (0,) + across)])
    units_b = gather_back(own, [(0,) + across, (2,) + beside])
    down_b = place_down(map_b, inverse_b, tiles // 2, crossed, part, hidden_width)
    flat = (2 * n_ep * tok_dev, hidden_width)
    units = [units_a.reshape(flat), units_b.reshape(flat)]
    product = down_product(
        [down_a, down_b], units, factors, tile_rows * largest_divisor(row_tiles, 2)
    )
    bits = [half]
    while bits[0] > 1:
        bits.insert(0, bits[0] // 2)
    bits = [bits[0]] + bits[-2:0:-1] + [bits[-1]]
    product = product.reshape((2, 2) + (2,) * (len(bits) - 1) + (tok_dev, part))
    sums = [None, None]
    for d in (1, 0):
        total = product[d]
        for bit in bits[:-1]:
            total = plain_sum(total[:, 0], flip(total[:, 1], "ep", bit))
        sums[d] = plain_sum(total[0], flip(total[1], "ep", bits[-1]))
    mine, other = sums[0], flip(sums[1], *across)
    mixed = jnp.where(
        side == 0,
        jnp.concatenate([mine, other], axis=1),
        jnp.concatenate([other, mine], axis=1),
    ).astype(jnp.float32)
    layer_out = (values + mixed).astype(jnp.bfloat16)
    stream = layer_out.astype(jnp.float32)
    renorm = lax.rsqrt(jnp.mean(stream * stream, axis=1, keepdims=True) + 1e-06)
    next_normed = (stream * renorm).astype(jnp.bfloat16)
    whole_router = jnp.where(
        side == 0,
        jnp.concatenate([next_router, other_router], axis=0),
        jnp.concatenate([other_router, next_router], axis=0),
    )
    next_logits = jnp.dot(next_normed, whole_router, preferred_element_type=jnp.float32)
    return (layer_out, jax.nn.sigmoid(next_logits))


def sparse_layer(tokens, norm_gain, router, next_router, expert_ids, store, send_list, cache_map):
    tok_dev, width = tokens.shape
    n_dp = lax.axis_size("dp")
    experts = router.shape[1]
    top = expert_ids.shape[1]
    tiles = cache_map.shape[1]
    tile_rows = store.shape[3]
    tile_cols = store.shape[4]
    part = width // n_dp
    row_tiles = part // tile_rows
    col_tiles = tiles // (2 * row_tiles)
    hidden_width = col_tiles * tile_cols
    capacity = row_capacity(tokens, router, expert_ids)
    values = tokens.astype(jnp.float32)
    scale = lax.rsqrt(jnp.mean(values * values, axis=1, keepdims=True) + 1e-06)
    normed = (values * scale * norm_gain).astype(jnp.bfloat16)
    scores = jax.nn.sigmoid(jnp.dot(normed, router, preferred_element_type=jnp.float32))
    chosen = (expert_ids[:, :, None] == jnp.arange(experts, dtype=jnp.int32)[None, None, :]).astype(
        jnp.float32
    )
    picked = jnp.sum(chosen * scores[:, None, :], axis=2)
    weights = (2.5 * picked / jnp.sum(picked, axis=1, keepdims=True)).astype(jnp.bfloat16)
    flat = chosen.reshape(tok_dev * top, experts)
    before = jnp.cumsum(flat, axis=0) - flat
    rank = jnp.sum(before * flat, axis=1).astype(jnp.int32)
    slot = expert_ids.reshape(-1) * capacity + rank
    columns = jnp.arange(experts * capacity, dtype=jnp.int32)
    match = (slot[:, None] == columns[None, :]).reshape(tok_dev, top, experts * capacity)
    dispatch = jnp.sum(match.astype(jnp.float32), axis=1).astype(jnp.bfloat16)
    combine = jnp.sum(
        jnp.where(match, weights.astype(jnp.float32)[:, :, None], 0.0), axis=1
    ).astype(jnp.bfloat16)
    outgoing = lax.dot_general(
        dispatch, normed, (((0,), (0,)), ((), ())), preferred_element_type=jnp.float32
    ).astype(jnp.bfloat16)
    owned = store.reshape(store.shape[2], tile_rows, tile_cols)
    leaving = owned[jnp.maximum(send_list.reshape(-1), 0)]
    arrived = lax.all_to_all(leaving, "ep", split_axis=0, concat_axis=0, tiled=True)
    cached = arrived[cache_map.reshape(-1)].reshape(2, row_tiles, col_tiles, tile_rows, tile_cols)
    up_tiles = cached[0]
    down_tiles = cached[1]
    rows = lax.all_to_all(
        lax.all_to_all(outgoing, "ep", split_axis=0, concat_axis=0, tiled=True),
        "dp",
        split_axis=1,
        concat_axis=0,
        tiled=True,
    )
    count = rows.shape[0]
    block = rows.reshape(count, row_tiles, tile_rows)
    product = jnp.einsum("nat,acts->ncs", block, up_tiles, preferred_element_type=jnp.float32)
    summed = lax.psum(product.reshape(count, hidden_width).astype(jnp.bfloat16), "dp").astype(
        jnp.float32
    )
    hidden = jax.nn.silu(summed).astype(jnp.bfloat16)
    number = hidden.shape[0]
    product = jnp.einsum(
        "ncs,acts->nat",
        hidden.reshape(number, col_tiles, tile_cols),
        down_tiles,
        preferred_element_type=jnp.float32,
    )
    result = product.reshape(number, part).astype(jnp.bfloat16)
    back = lax.all_to_all(
        lax.all_to_all(result, "dp", split_axis=0, concat_axis=1, tiled=True),
        "ep",
        split_axis=0,
        concat_axis=0,
        tiled=True,
    )
    mixed = jnp.dot(combine, back, preferred_element_type=jnp.float32)
    layer_out = (values + mixed).astype(jnp.bfloat16)
    stream = layer_out.astype(jnp.float32)
    renorm = lax.rsqrt(jnp.mean(stream * stream, axis=1, keepdims=True) + 1e-06)
    next_normed = (stream * renorm).astype(jnp.bfloat16)
    features = lax.all_to_all(next_normed, "dp", split_axis=1, concat_axis=0, tiled=True)
    partial_scores = jnp.dot(features, next_router, preferred_element_type=jnp.float32)
    next_logits = lax.psum_scatter(
        partial_scores.astype(jnp.bfloat16), "dp", scatter_dimension=0, tiled=True
    ).astype(jnp.float32)
    return (layer_out, jax.nn.sigmoid(next_logits))


def row_capacity(tokens, router, expert_ids):
    tok_dev, experts, top = tokens.shape[0], router.shape[1], expert_ids.shape[1]
    return min(tok_dev, max(2, 2 * tok_dev * top // experts))


def per_device(*arrays):
    tokens, _, router, _, expert_ids, store, _, cache_map = arrays
    n_ep = lax.axis_size("ep")
    every_row = row_capacity(tokens, router, expert_ids) == tokens.shape[0]
    one_each = router.shape[1] == n_ep and store.shape[2] == cache_map.shape[1]
    two_power = n_ep > 2 and n_ep & (n_ep - 1) == 0
    one_each = one_each and cache_map.shape[1] % (2 * n_ep) == 0
    if every_row and one_each and two_power and lax.axis_size("dp") == 2:
        return dense_layer(*arrays)
    return sparse_layer(*arrays)


def solution(mesh):
    in_specs = (
        P(("ep", "dp"), None),
        P(),
        P(),
        P("dp", None),
        P(("ep", "dp"), None),
        P("ep", "dp", None, None, None),
        P("ep", None),
        P("ep", None),
    )
    out_specs = (P(("ep", "dp"), None), P(("ep", "dp"), None))
    return jax.shard_map(
        per_device, mesh=mesh, in_specs=in_specs, out_specs=out_specs, check_vma=False
    )
```

```python
import functools

import jax
import jax.numpy as jnp
from jax import lax
from jax.experimental import pallas as pl
from jax.experimental.pallas import tpu as pltpu
from jax.sharding import PartitionSpec as P


ANY = pl.BlockSpec(memory_space=pl.ANY)
VMEM = pl.BlockSpec(memory_space=pltpu.VMEM)
SMEM = pl.BlockSpec(memory_space=pltpu.SMEM)


def largest_divisor(number, most):
    return max(d for d in range(1, most + 1) if number % d == 0)


def pick_kernel(column_of, chunks, size, place_ref, list_ref, store_ref, *refs):
    outs, (held, in_sems, out_sem) = refs[:-3], refs[-3:]
    place = place_ref[0]
    for chunk in range(chunks):

        def fetch(i, carry, chunk=chunk):
            tile = list_ref[column_of(place, chunk, i)]
            copy = pltpu.make_async_copy(
                store_ref.at[tile], held.at[chunk * size + i], in_sems.at[chunk]
            )
            copy.start()
            return carry

        lax.fori_loop(0, size, fetch, 0)
    puts = []
    for chunk in range(chunks):
        block = held.at[pl.ds(chunk * size, size)]
        pltpu.make_async_copy(block, block, in_sems.at[chunk]).wait()
        target = outs[chunk] if len(outs) > 1 else outs[0].at[pl.ds(chunk * size, size)]
        puts.append(pltpu.make_async_copy(block, target, out_sem.at[chunk]))
        puts[-1].start()
    for put in puts:
        put.wait()


def pick_tiles(column_of, place, wanted, store, chunks, size, joined):
    tile = store.shape[1:]
    if joined:
        shapes = jax.ShapeDtypeStruct((chunks * size,) + tile, store.dtype)
    else:
        shapes = [jax.ShapeDtypeStruct((size,) + tile, store.dtype)] * chunks
    return pl.pallas_call(
        functools.partial(pick_kernel, column_of, chunks, size),
        out_shape=shapes,
        in_specs=[SMEM, SMEM, ANY],
        out_specs=ANY if joined else [ANY] * chunks,
        scratch_shapes=[
            pltpu.VMEM((chunks * size,) + tile, store.dtype),
            pltpu.SemaphoreType.DMA((chunks,)),
            pltpu.SemaphoreType.DMA((chunks,)),
        ],
        cost_estimate=pl.CostEstimate(
            flops=chunks * size * 2**24, bytes_accessed=chunks * size * 2**17, transcendentals=0
        ),
    )(place, wanted, store)


def scatter_tiles(first, map_ref, tile_refs, sources, weight, sem_of):
    tile_rows, tile_cols = sources[0].shape[1:]
    part, width = weight.shape
    row_tiles, col_tiles = part // tile_rows, width // tile_cols

    def place_of(s):
        row, column = lax.div(s, col_tiles), lax.rem(s, col_tiles)
        rows = pl.ds(pl.multiple_of(row * tile_rows, tile_rows), tile_rows)
        columns = pl.ds(pl.multiple_of(column * tile_cols, tile_cols), tile_cols)
        return row, column, weight.at[rows, columns]

    begin = 0
    for source in sources:

        def fetch(i, carry, source=source, begin=begin):
            s = tile_refs[begin + i] - first

            @pl.when((s >= 0) & (s < row_tiles * col_tiles))
            def _():
                row, column, place = place_of(s)
                pltpu.make_async_copy(source.at[i], place, sem_of(row, column)).start()

            return carry

        lax.fori_loop(0, source.shape[0], fetch, 0, unroll=source.shape[0] < 8)
        begin += source.shape[0]

    def clear(row, carry):
        for column in range(col_tiles):

            @pl.when(map_ref[first + row * col_tiles + column] < 0)
            def _(column=column):
                rows = pl.ds(pl.multiple_of(row * tile_rows, tile_rows), tile_rows)
                weight[rows, pl.ds(column * tile_cols, tile_cols)] = jnp.zeros(
                    (tile_rows, tile_cols), weight.dtype
                )

        return carry

    lax.fori_loop(0, row_tiles, clear, 0)


def wait_tiles(first, map_ref, weight, tile, sem, rows, columns):
    tile_rows, tile_cols = tile
    col_tiles = weight.shape[1] // tile_cols

    def wait(i, carry):
        row = rows[0] + i
        for column in columns:

            @pl.when(map_ref[first + row * col_tiles + column] >= 0)
            def _(column=column):
                place = weight.at[
                    pl.ds(pl.multiple_of(row * tile_rows, tile_rows), tile_rows),
                    pl.ds(column * tile_cols, tile_cols),
                ]
                pltpu.make_async_copy(place, place, sem).wait()

        return carry

    lax.fori_loop(0, rows[1], wait, 0)


def up_kernel(step, size, map_ref, tile_refs, rows_ref, *refs):
    sources = refs[:-6]
    keep_ref, send_ref, rows, weight, rows_sem, sems = refs[-6:]
    tile = sources[0].shape[1:]
    part, width = weight.shape
    row_tiles, col_tiles = part // tile[0], width // tile[1]
    fetch = pltpu.make_async_copy(rows_ref.at[:, pl.ds(0, part)], rows, rows_sem)
    fetch.start()
    scatter_tiles(
        0, map_ref, tile_refs, sources, weight, lambda row, column: sems.at[lax.div(column, step)]
    )
    fetch.wait()
    for block in range(col_tiles // step):
        wait_tiles(
            0,
            map_ref,
            weight,
            tile,
            sems.at[block],
            (0, row_tiles),
            range(block * step, block * step + step),
        )
        columns = pl.ds(block * step * tile[1], step * tile[1])
        product = jnp.dot(
            rows[...], weight[:, columns], preferred_element_type=jnp.float32
        ).astype(keep_ref.dtype)
        for i in range(product.shape[0] // (2 * size)):
            place = pl.ds(i * size, size)
            keep_ref[place, columns] = product[2 * i * size : (2 * i + 1) * size]
            send_ref[place, columns] = product[(2 * i + 1) * size : (2 * i + 2) * size]


def up_product(index, inverse, rows, sources, part, width, size):
    tile_cols = sources[0].shape[2]
    step = largest_divisor(width // tile_cols, 4)
    count = rows.shape[0]
    return pl.pallas_call(
        functools.partial(up_kernel, step, size),
        out_shape=[jax.ShapeDtypeStruct((count // 2, width), jnp.bfloat16)] * 2,
        in_specs=[SMEM, SMEM] + [ANY] * (1 + len(sources)),
        out_specs=[VMEM, VMEM],
        scratch_shapes=[
            pltpu.VMEM((count, part), rows.dtype),
            pltpu.VMEM((part, width), sources[0].dtype),
            pltpu.SemaphoreType.DMA,
            pltpu.SemaphoreType.DMA((width // tile_cols // step,)),
        ],
        cost_estimate=pl.CostEstimate(
            flops=2 * count * part * width,
            bytes_accessed=2 * (part * width + count * (part + width)),
            transcendentals=0,
        ),
        name="up_product",
    )(index, inverse, rows, *sources)


def place_kernel(first, chunks, map_ref, tile_refs, *refs):
    sources, (out_ref, weight, in_sems, out_sems) = refs[:-4], refs[-4:]
    tile = sources[0].shape[1:]
    part, width = weight.shape
    size = part // tile[0] // chunks
    scatter_tiles(
        first, map_ref, tile_refs, sources, weight, lambda row, column: in_sems.at[lax.div(row, size)]
    )
    puts = []
    for chunk in range(chunks):
        wait_tiles(
            first,
            map_ref,
            weight,
            tile,
            in_sems.at[chunk],
            (chunk * size, size),
            range(width // tile[1]),
        )
        block = pl.ds(chunk * size * tile[0], size * tile[0])
        puts.append(pltpu.make_async_copy(weight.at[block], out_ref.at[block], out_sems.at[chunk]))
        puts[-1].start()
    for put in puts:
        put.wait()


def place_down(index, inverse, first, sources, part, width):
    chunks = largest_divisor(part // sources[0].shape[1], 4)
    return pl.pallas_call(
        functools.partial(place_kernel, first, chunks),
        out_shape=jax.ShapeDtypeStruct((part, width), sources[0].dtype),
        in_specs=[SMEM, SMEM] + [ANY] * len(sources),
        out_specs=ANY,
        scratch_shapes=[
            pltpu.VMEM((part, width), sources[0].dtype),
            pltpu.SemaphoreType.DMA((chunks,)),
            pltpu.SemaphoreType.DMA((chunks,)),
        ],
        cost_estimate=pl.CostEstimate(
            flops=part * width * 1024, bytes_accessed=4 * part * width, transcendentals=0
        ),
        name="place_down",
    )(index, inverse, *sources)


def down_kernel(sizes, split, *refs):
    experts = len(sizes)
    outs, held = refs[4 * experts : -1], refs[-1]

    @pl.when(pl.program_id(0) == 0)
    def _():
        for e, size in enumerate(sizes):
            for which in range(2):
                units = refs[4 * e + 1 + which]
                for i in range(units.shape[0] // size):
                    place = pl.ds((2 * i + which) * size, size)
                    held[e, place, :] = units[pl.ds(i * size, size), :]

    total = 0.0
    for e in range(experts):
        weight, factor = refs[4 * e], refs[4 * e + 3]
        product = lax.dot_general(
            held[e], weight[...], (((1,), (1,)), ((), ())), preferred_element_type=jnp.float32
        )
        total = total + product * factor[...]
    total = total.astype(outs[0].dtype)
    count = total.shape[0] // 2
    for d in range(2):
        for i in range(count // (2 * split)):
            for which in range(2):
                begin = d * count + (2 * i + which) * split
                outs[2 * d + which][pl.ds(i * split, split), :] = total[begin : begin + split]


def down_product(weights, units, sizes, factors, block, split):
    part, width = weights[0].shape
    count = factors[0].shape[0]
    specs, operands = [], []
    for weight, (first, second), factor in zip(weights, units, factors, strict=True):
        specs += [
            pl.BlockSpec((block, width), lambda i: (i, 0)),
            pl.BlockSpec((count // 2, width), lambda i: (0, 0)),
            pl.BlockSpec((count // 2, width), lambda i: (0, 0)),
            pl.BlockSpec((count, 1), lambda i: (0, 0)),
        ]
        operands += [weight, first, second, factor]
    return pl.pallas_call(
        functools.partial(down_kernel, sizes, split),
        grid=(part // block,),
        out_shape=[jax.ShapeDtypeStruct((count // 4, part), jnp.bfloat16)] * 4,
        in_specs=specs,
        out_specs=[pl.BlockSpec((count // 4, block), lambda i: (0, i))] * 4,
        scratch_shapes=[pltpu.VMEM((len(weights), count, width), jnp.bfloat16)],
        cost_estimate=pl.CostEstimate(
            flops=2 * len(weights) * count * part * width,
            bytes_accessed=2 * (len(weights) * (part + count) * width + count * part),
            transcendentals=0,
        ),
        name="down_product",
    )(*operands)


def flip(value, axis, bit):
    return lax.ppermute(value, axis, [(i, i ^ bit) for i in range(lax.axis_size(axis))])


def silu_sum(first, second):
    pre = first.astype(jnp.float32) + second.astype(jnp.float32)
    return (pre * jax.nn.sigmoid(pre)).astype(jnp.bfloat16)


def plain_sum(first, second):
    return (first.astype(jnp.float32) + second.astype(jnp.float32)).astype(jnp.bfloat16)


def dense_layer(tokens, norm_gain, router, next_router, expert_ids, store, send_list, cache_map):
    tok_dev, width = tokens.shape
    n_ep = lax.axis_size("ep")
    half = n_ep // 2
    experts = router.shape[1]
    tiles = cache_map.shape[1]
    lanes_of = tiles // n_ep
    sub = lanes_of // 2
    tile_rows, tile_cols = store.shape[3:]
    part = width // 2
    row_tiles = part // tile_rows
    col_tiles = tiles // (2 * row_tiles)
    hidden_width = col_tiles * tile_cols
    me, side = lax.axis_index("ep"), lax.axis_index("dp")
    groups = [list(range(half)), list(range(half, n_ep))]
    mirror = ("ep", half)
    beside = ("ep", 1)
    across = ("dp", 1)

    owned = store.reshape(tiles, tile_rows, tile_cols)
    wanted = send_list.reshape(-1)
    place = jnp.reshape(me, (1,)).astype(jnp.int32)

    def near_column(number, i, lane):
        return i * lanes_of + lane

    def far_column(number, j, lane):
        return half * lanes_of + sub * (number ^ j) + lane

    leaving = pick_tiles(near_column, place, wanted, owned, half, lanes_of, True)
    far = pick_tiles(far_column, place, wanted, owned, n_ep, sub, False)

    values = tokens.astype(jnp.float32)
    scale = lax.rsqrt(jnp.mean(values * values, axis=1, keepdims=True) + 1e-06)
    normed = (values * scale * norm_gain).astype(jnp.bfloat16)
    scores = jax.nn.sigmoid(jnp.dot(normed, router, preferred_element_type=jnp.float32))
    chosen = (
        expert_ids[:, :, None] == jnp.arange(experts, dtype=jnp.int32)[None, None, :]
    ).astype(jnp.float32)
    picked = jnp.sum(chosen, axis=1) * scores
    weights = (2.5 * picked / jnp.sum(picked, axis=1, keepdims=True)).astype(jnp.bfloat16)
    digit = tile_cols
    each = -(-tiles // tok_dev)
    codes = jnp.pad(cache_map.reshape(-1), (0, each * tok_dev - tiles)).reshape(tok_dev, each)
    codes = jnp.concatenate([codes // digit, codes % digit], axis=1).astype(jnp.bfloat16)
    used = experts + 2 * each
    lanes = tile_cols * (-(-used // tile_cols))
    first, second = normed[:, :part], normed[:, part:]
    mine = jnp.concatenate(
        [
            jnp.where(side == 0, first, second),
            jnp.pad(jnp.concatenate([weights, codes], axis=1), ((0, 0), (0, lanes - used))),
        ],
        axis=1,
    )
    theirs = jnp.concatenate(
        [
            jnp.where(side == 0, second, first),
            jnp.pad(weights, ((0, 0), (0, lanes - experts))),
        ],
        axis=1,
    )
    rows = jnp.stack([mine, flip(theirs, *across)])
    arrived = lax.all_to_all(
        leaving, "ep", split_axis=0, concat_axis=0, tiled=True, axis_index_groups=groups
    )
    rows = jnp.stack([rows, flip(rows, *mirror)], axis=1)
    blocks = [rows]
    for number in range(2, half, 2):
        blocks.append(flip(rows, "ep", number))
    crossed = [far[0]]
    for j in range(1, n_ep):
        crossed.append(flip(far[j], "ep", j))
    rows = jnp.stack(blocks, axis=2)
    rows = jnp.stack([rows, flip(rows, *beside)], axis=2)
    rows = rows.reshape(2 * n_ep * tok_dev, part + lanes)
    rows, other_router = lax.optimization_barrier((rows, flip(next_router, *across)))

    def map_of(number):
        relative = number ^ me
        block = (relative // half * 2 + relative % 2) * (half // 2) + relative % half // 2
        got = lax.dynamic_slice(
            rows, (block * tok_dev, part + experts), (tok_dev, 2 * each)
        ).astype(jnp.int32)
        return (got[:, :each] * digit + got[:, each:]).reshape(-1)[:tiles]

    lane = lax.broadcasted_iota(jnp.int32, (1, lanes), 1)
    gates = rows[:, part:].astype(jnp.float32)
    expert_of = [me % half, half + me // 2]
    factors = [
        jnp.sum(jnp.where(lane == e, gates, 0.0), axis=1, keepdims=True) for e in expert_of
    ]

    slots = map_of(expert_of[0])
    owner, number = slots // lanes_of, slots % lanes_of
    near = (owner // half) == (me // half)
    map_a = jnp.where(near, owner % half * lanes_of + number, -1)
    slots = map_of(expert_of[1])
    owner, inside = slots // lanes_of, slots % lanes_of - sub * (me % 2)
    map_b = jnp.where((inside >= 0) & (inside < sub), (owner ^ me) * sub + inside, -1)

    def inverse_of(index):
        held = index[None, :] == jnp.arange(tiles // 2, dtype=jnp.int32)[:, None]
        number = jnp.arange(1, tiles + 1, dtype=jnp.int32)[None, :]
        return jnp.sum(jnp.where(held, number, 0), axis=1) - 1

    held_a = (map_a, inverse_of(map_a))
    held_b = (map_b, inverse_of(map_b))
    (map_a, inverse_a), (map_b, inverse_b) = lax.optimization_barrier((held_a, held_b))
    quarter = half * tok_dev
    keep, send = up_product(map_a, inverse_a, rows, [arrived], part, hidden_width, 2 * quarter)
    own = plain_sum(keep, flip(send, *across))
    down_a = place_down(map_a, inverse_a, tiles // 2, [arrived], part, hidden_width)
    own = silu_sum(own[:quarter], flip(own[quarter:], *mirror))
    kept, crossed, down_a, factors = lax.optimization_barrier((own, crossed, down_a, factors))
    own = jnp.concatenate([kept, flip(own, *across)], axis=0)
    units_a = (own, flip(own, *mirror))

    eighth = half // 2 * tok_dev
    keep, send = up_product(map_b, inverse_b, rows, crossed, part, hidden_width, eighth)
    own = plain_sum(keep, flip(send, *beside))
    own = silu_sum(own[:quarter], flip(own[quarter:], *across))
    own = jnp.concatenate([own, flip(own, *across)], axis=0)
    units_b = (own, flip(own, *beside))
    down_b = place_down(map_b, inverse_b, tiles // 2, crossed, part, hidden_width)

    products = down_product(
        [down_a, down_b],
        [units_a, units_b],
        (quarter, eighth),
        factors,
        tile_rows * largest_divisor(row_tiles, 2),
        eighth,
    )
    sums = [None, None]
    for d in (1, 0):
        total = plain_sum(products[2 * d], flip(products[2 * d + 1], *beside))
        total = total.reshape(2, half // 2, tok_dev, part)
        pieces = [total[:, 0]]
        for m in range(1, half // 2):
            pieces.append(flip(total[:, m], "ep", 2 * m))
        total = sum(piece.astype(jnp.float32) for piece in pieces).astype(jnp.bfloat16)
        sums[d] = plain_sum(total[0], flip(total[1], *mirror))
    mine, other = sums[0], flip(sums[1], *across)
    mixed = jnp.where(
        side == 0,
        jnp.concatenate([mine, other], axis=1),
        jnp.concatenate([other, mine], axis=1),
    ).astype(jnp.float32)
    layer_out = (values + mixed).astype(jnp.bfloat16)
    stream = layer_out.astype(jnp.float32)
    renorm = lax.rsqrt(jnp.mean(stream * stream, axis=1, keepdims=True) + 1e-06)
    next_normed = (stream * renorm).astype(jnp.bfloat16)
    whole_router = jnp.where(
        side == 0,
        jnp.concatenate([next_router, other_router], axis=0),
        jnp.concatenate([other_router, next_router], axis=0),
    )
    next_logits = jnp.dot(next_normed, whole_router, preferred_element_type=jnp.float32)
    return (layer_out, jax.nn.sigmoid(next_logits))


def sparse_layer(tokens, norm_gain, router, next_router, expert_ids, store, send_list, cache_map):
    tok_dev, width = tokens.shape
    n_dp = lax.axis_size("dp")
    experts = router.shape[1]
    top = expert_ids.shape[1]
    tiles = cache_map.shape[1]
    tile_rows = store.shape[3]
    tile_cols = store.shape[4]
    part = width // n_dp
    row_tiles = part // tile_rows
    col_tiles = tiles // (2 * row_tiles)
    hidden_width = col_tiles * tile_cols
    capacity = row_capacity(tokens, router, expert_ids)
    values = tokens.astype(jnp.float32)
    scale = lax.rsqrt(jnp.mean(values * values, axis=1, keepdims=True) + 1e-06)
    normed = (values * scale * norm_gain).astype(jnp.bfloat16)
    scores = jax.nn.sigmoid(jnp.dot(normed, router, preferred_element_type=jnp.float32))
    chosen = (expert_ids[:, :, None] == jnp.arange(experts, dtype=jnp.int32)[None, None, :]).astype(
        jnp.float32
    )
    picked = jnp.sum(chosen * scores[:, None, :], axis=2)
    weights = (2.5 * picked / jnp.sum(picked, axis=1, keepdims=True)).astype(jnp.bfloat16)
    flat = chosen.reshape(tok_dev * top, experts)
    before = jnp.cumsum(flat, axis=0) - flat
    rank = jnp.sum(before * flat, axis=1).astype(jnp.int32)
    slot = expert_ids.reshape(-1) * capacity + rank
    columns = jnp.arange(experts * capacity, dtype=jnp.int32)
    match = (slot[:, None] == columns[None, :]).reshape(tok_dev, top, experts * capacity)
    dispatch = jnp.sum(match.astype(jnp.float32), axis=1).astype(jnp.bfloat16)
    combine = jnp.sum(
        jnp.where(match, weights.astype(jnp.float32)[:, :, None], 0.0), axis=1
    ).astype(jnp.bfloat16)
    outgoing = lax.dot_general(
        dispatch, normed, (((0,), (0,)), ((), ())), preferred_element_type=jnp.float32
    ).astype(jnp.bfloat16)
    owned = store.reshape(store.shape[2], tile_rows, tile_cols)
    leaving = owned[jnp.maximum(send_list.reshape(-1), 0)]
    arrived = lax.all_to_all(leaving, "ep", split_axis=0, concat_axis=0, tiled=True)
    cached = arrived[cache_map.reshape(-1)].reshape(2, row_tiles, col_tiles, tile_rows, tile_cols)
    up_tiles = cached[0]
    down_tiles = cached[1]
    rows = lax.all_to_all(
        lax.all_to_all(outgoing, "ep", split_axis=0, concat_axis=0, tiled=True),
        "dp",
        split_axis=1,
        concat_axis=0,
        tiled=True,
    )
    count = rows.shape[0]
    block = rows.reshape(count, row_tiles, tile_rows)
    product = jnp.einsum("nat,acts->ncs", block, up_tiles, preferred_element_type=jnp.float32)
    summed = lax.psum(product.reshape(count, hidden_width).astype(jnp.bfloat16), "dp").astype(
        jnp.float32
    )
    hidden = jax.nn.silu(summed).astype(jnp.bfloat16)
    number = hidden.shape[0]
    product = jnp.einsum(
        "ncs,acts->nat",
        hidden.reshape(number, col_tiles, tile_cols),
        down_tiles,
        preferred_element_type=jnp.float32,
    )
    result = product.reshape(number, part).astype(jnp.bfloat16)
    back = lax.all_to_all(
        lax.all_to_all(result, "dp", split_axis=0, concat_axis=1, tiled=True),
        "ep",
        split_axis=0,
        concat_axis=0,
        tiled=True,
    )
    mixed = jnp.dot(combine, back, preferred_element_type=jnp.float32)
    layer_out = (values + mixed).astype(jnp.bfloat16)
    stream = layer_out.astype(jnp.float32)
    renorm = lax.rsqrt(jnp.mean(stream * stream, axis=1, keepdims=True) + 1e-06)
    next_normed = (stream * renorm).astype(jnp.bfloat16)
    features = lax.all_to_all(next_normed, "dp", split_axis=1, concat_axis=0, tiled=True)
    partial_scores = jnp.dot(features, next_router, preferred_element_type=jnp.float32)
    next_logits = lax.psum_scatter(
        partial_scores.astype(jnp.bfloat16), "dp", scatter_dimension=0, tiled=True
    ).astype(jnp.float32)
    return (layer_out, jax.nn.sigmoid(next_logits))


def row_capacity(tokens, router, expert_ids):
    tok_dev, experts, top = tokens.shape[0], router.shape[1], expert_ids.shape[1]
    return min(tok_dev, max(2, 2 * tok_dev * top // experts))


def per_device(*arrays):
    tokens, _, router, _, expert_ids, store, _, cache_map = arrays
    n_ep = lax.axis_size("ep")
    every_row = row_capacity(tokens, router, expert_ids) == tokens.shape[0]
    one_each = router.shape[1] == n_ep and store.shape[2] == cache_map.shape[1]
    two_power = n_ep > 2 and n_ep & (n_ep - 1) == 0
    one_each = one_each and cache_map.shape[1] % (2 * n_ep) == 0
    if every_row and one_each and two_power and lax.axis_size("dp") == 2:
        return dense_layer(*arrays)
    return sparse_layer(*arrays)


def solution(mesh):
    in_specs = (
        P(("ep", "dp"), None),
        P(),
        P(),
        P("dp", None),
        P(("ep", "dp"), None),
        P("ep", "dp", None, None, None),
        P("ep", None),
        P("ep", None),
    )
    out_specs = (P(("ep", "dp"), None), P(("ep", "dp"), None))
    return jax.shard_map(
        per_device, mesh=mesh, in_specs=in_specs, out_specs=out_specs, check_vma=False
    )
```

```python
import functools

import jax
import jax.numpy as jnp
from jax import lax
from jax.experimental import pallas as pl
from jax.experimental.pallas import tpu as pltpu
from jax.sharding import PartitionSpec as P


ANY = pl.BlockSpec(memory_space=pl.ANY)
VMEM = pl.BlockSpec(memory_space=pltpu.VMEM)
SMEM = pl.BlockSpec(memory_space=pltpu.SMEM)


def largest_divisor(number, most):
    return max(d for d in range(1, most + 1) if number % d == 0)


def pick_kernel(column_of, chunks, size, place_ref, list_ref, store_ref, *refs):
    outs, (held, in_sems, out_sem) = refs[:-3], refs[-3:]
    place = place_ref[0]
    for chunk in range(chunks):

        def fetch(i, carry, chunk=chunk):
            tile = list_ref[column_of(place, chunk, i)]
            copy = pltpu.make_async_copy(
                store_ref.at[tile], held.at[chunk * size + i], in_sems.at[chunk]
            )
            copy.start()
            return carry

        lax.fori_loop(0, size, fetch, 0)
    puts = []
    for chunk in range(chunks):
        block = held.at[pl.ds(chunk * size, size)]
        pltpu.make_async_copy(block, block, in_sems.at[chunk]).wait()
        target = outs[chunk] if len(outs) > 1 else outs[0].at[pl.ds(chunk * size, size)]
        puts.append(pltpu.make_async_copy(block, target, out_sem.at[chunk]))
        puts[-1].start()
    for put in puts:
        put.wait()


def pick_tiles(column_of, place, wanted, store, chunks, size, joined):
    tile = store.shape[1:]
    if joined:
        shapes = jax.ShapeDtypeStruct((chunks * size,) + tile, store.dtype)
    else:
        shapes = [jax.ShapeDtypeStruct((size,) + tile, store.dtype)] * chunks
    return pl.pallas_call(
        functools.partial(pick_kernel, column_of, chunks, size),
        out_shape=shapes,
        in_specs=[SMEM, SMEM, ANY],
        out_specs=ANY if joined else [ANY] * chunks,
        scratch_shapes=[
            pltpu.VMEM((chunks * size,) + tile, store.dtype),
            pltpu.SemaphoreType.DMA((chunks,)),
            pltpu.SemaphoreType.DMA((chunks,)),
        ],
        cost_estimate=pl.CostEstimate(
            flops=chunks * size * 2**24, bytes_accessed=chunks * size * 2**17, transcendentals=0
        ),
    )(place, wanted, store)


def scatter_tiles(first, map_ref, tile_refs, sources, weight, sem_of):
    tile_rows, tile_cols = sources[0].shape[1:]
    part, width = weight.shape
    row_tiles, col_tiles = part // tile_rows, width // tile_cols

    def place_of(s):
        row, column = lax.div(s, col_tiles), lax.rem(s, col_tiles)
        rows = pl.ds(pl.multiple_of(row * tile_rows, tile_rows), tile_rows)
        columns = pl.ds(pl.multiple_of(column * tile_cols, tile_cols), tile_cols)
        return row, column, weight.at[rows, columns]

    begin = 0
    for source in sources:

        def fetch(i, carry, source=source, begin=begin):
            s = tile_refs[begin + i] - first

            @pl.when((s >= 0) & (s < row_tiles * col_tiles))
            def _():
                row, column, place = place_of(s)
                pltpu.make_async_copy(source.at[i], place, sem_of(row, column)).start()

            return carry

        lax.fori_loop(0, source.shape[0], fetch, 0, unroll=source.shape[0] < 8)
        begin += source.shape[0]

    def clear(row, carry):
        for column in range(col_tiles):

            @pl.when(map_ref[first + row * col_tiles + column] < 0)
            def _(column=column):
                rows = pl.ds(pl.multiple_of(row * tile_rows, tile_rows), tile_rows)
                weight[rows, pl.ds(column * tile_cols, tile_cols)] = jnp.zeros(
                    (tile_rows, tile_cols), weight.dtype
                )

        return carry

    lax.fori_loop(0, row_tiles, clear, 0)


def wait_tiles(first, map_ref, weight, tile, sem, rows, columns):
    tile_rows, tile_cols = tile
    col_tiles = weight.shape[1] // tile_cols

    def wait(i, carry):
        row = rows[0] + i
        for column in columns:

            @pl.when(map_ref[first + row * col_tiles + column] >= 0)
            def _(column=column):
                place = weight.at[
                    pl.ds(pl.multiple_of(row * tile_rows, tile_rows), tile_rows),
                    pl.ds(column * tile_cols, tile_cols),
                ]
                pltpu.make_async_copy(place, place, sem).wait()

        return carry

    lax.fori_loop(0, rows[1], wait, 0)


def up_kernel(step, size, map_ref, tile_refs, rows_ref, *refs):
    sources = refs[:-6]
    keep_ref, send_ref, rows, weight, rows_sem, sems = refs[-6:]
    tile = sources[0].shape[1:]
    part, width = weight.shape
    row_tiles, col_tiles = part // tile[0], width // tile[1]
    fetch = pltpu.make_async_copy(rows_ref.at[:, pl.ds(0, part)], rows, rows_sem)
    fetch.start()
    scatter_tiles(
        0, map_ref, tile_refs, sources, weight, lambda row, column: sems.at[lax.div(column, step)]
    )
    fetch.wait()
    for block in range(col_tiles // step):
        wait_tiles(
            0,
            map_ref,
            weight,
            tile,
            sems.at[block],
            (0, row_tiles),
            range(block * step, block * step + step),
        )
        columns = pl.ds(block * step * tile[1], step * tile[1])
        product = jnp.dot(
            rows[...], weight[:, columns], preferred_element_type=jnp.float32
        ).astype(keep_ref.dtype)
        for i in range(product.shape[0] // (2 * size)):
            place = pl.ds(i * size, size)
            keep_ref[place, columns] = product[2 * i * size : (2 * i + 1) * size]
            send_ref[place, columns] = product[(2 * i + 1) * size : (2 * i + 2) * size]


def up_product(index, inverse, rows, sources, part, width, size):
    tile_cols = sources[0].shape[2]
    step = largest_divisor(width // tile_cols, 4)
    count = rows.shape[0]
    return pl.pallas_call(
        functools.partial(up_kernel, step, size),
        out_shape=[jax.ShapeDtypeStruct((count // 2, width), jnp.bfloat16)] * 2,
        in_specs=[SMEM, SMEM] + [ANY] * (1 + len(sources)),
        out_specs=[VMEM, VMEM],
        scratch_shapes=[
            pltpu.VMEM((count, part), rows.dtype),
            pltpu.VMEM((part, width), sources[0].dtype),
            pltpu.SemaphoreType.DMA,
            pltpu.SemaphoreType.DMA((width // tile_cols // step,)),
        ],
        cost_estimate=pl.CostEstimate(
            flops=2 * count * part * width,
            bytes_accessed=2 * (part * width + count * (part + width)),
            transcendentals=0,
        ),
        name="up_product",
    )(index, inverse, rows, *sources)


def place_kernel(first, chunks, map_ref, tile_refs, *refs):
    sources, (out_ref, weight, in_sems, out_sems) = refs[:-4], refs[-4:]
    tile = sources[0].shape[1:]
    part, width = weight.shape
    size = part // tile[0] // chunks
    scatter_tiles(
        first, map_ref, tile_refs, sources, weight, lambda row, column: in_sems.at[lax.div(row, size)]
    )
    puts = []
    for chunk in range(chunks):
        wait_tiles(
            first,
            map_ref,
            weight,
            tile,
            in_sems.at[chunk],
            (chunk * size, size),
            range(width // tile[1]),
        )
        block = pl.ds(chunk * size * tile[0], size * tile[0])
        puts.append(pltpu.make_async_copy(weight.at[block], out_ref.at[block], out_sems.at[chunk]))
        puts[-1].start()
    for put in puts:
        put.wait()


def place_down(index, inverse, first, sources, part, width):
    chunks = largest_divisor(part // sources[0].shape[1], 4)
    return pl.pallas_call(
        functools.partial(place_kernel, first, chunks),
        out_shape=jax.ShapeDtypeStruct((part, width), sources[0].dtype),
        in_specs=[SMEM, SMEM] + [ANY] * len(sources),
        out_specs=ANY,
        scratch_shapes=[
            pltpu.VMEM((part, width), sources[0].dtype),
            pltpu.SemaphoreType.DMA((chunks,)),
            pltpu.SemaphoreType.DMA((chunks,)),
        ],
        cost_estimate=pl.CostEstimate(
            flops=part * width * 1024, bytes_accessed=4 * part * width, transcendentals=0
        ),
        name="place_down",
    )(index, inverse, *sources)


def down_kernel(layout, split, number_ref, gate_ref, *refs):
    experts = number_ref.shape[0]
    weights, pieces = refs[:experts], refs[experts : experts + len(layout)]
    outs, held, factor = refs[experts + len(layout) : -2], refs[-2], refs[-1]

    @pl.when(pl.program_id(0) == 0)
    def _():
        gates = gate_ref[...].astype(jnp.float32)
        lane = lax.broadcasted_iota(jnp.int32, gates.shape, 1)
        for e in range(experts):
            mine = jnp.where(lane == number_ref[e], gates, 0.0)
            factor[e] = jnp.sum(mine, axis=1, keepdims=True)
        for units, (e, size, start, stride) in zip(pieces, layout, strict=True):
            for i in range(units.shape[0] // size):
                place = pl.ds(start + i * stride, size)
                held[e, place, :] = units[pl.ds(i * size, size), :]

    total = 0.0
    for e in range(experts):
        product = lax.dot_general(
            held[e], weights[e][...], (((1,), (1,)), ((), ())), preferred_element_type=jnp.float32
        )
        total = total + product * factor[e]
    total = total.astype(outs[0].dtype)
    count = total.shape[0] // 2
    for d in range(2):
        for i in range(count // (2 * split)):
            for which in range(2):
                begin = d * count + (2 * i + which) * split
                outs[2 * d + which][pl.ds(i * split, split), :] = total[begin : begin + split]


def down_product(weights, pieces, layout, numbers, rows, block, split):
    part, width = weights[0].shape
    count, lanes = rows.shape[0], rows.shape[1] - part
    specs = [SMEM, pl.BlockSpec((count, lanes), lambda i: (0, part // lanes))]
    specs += [pl.BlockSpec((block, width), lambda i: (i, 0))] * len(weights)
    specs += [pl.BlockSpec(piece.shape, lambda i: (0, 0)) for piece in pieces]
    return pl.pallas_call(
        functools.partial(down_kernel, layout, split),
        grid=(part // block,),
        out_shape=[jax.ShapeDtypeStruct((count // 4, part), jnp.bfloat16)] * 4,
        in_specs=specs,
        out_specs=[pl.BlockSpec((count // 4, block), lambda i: (0, i))] * 4,
        scratch_shapes=[
            pltpu.VMEM((len(weights), count, width), jnp.bfloat16),
            pltpu.VMEM((len(weights), count, 1), jnp.float32),
        ],
        cost_estimate=pl.CostEstimate(
            flops=2 * len(weights) * count * part * width,
            bytes_accessed=2 * (len(weights) * (part + count) * width + count * part),
            transcendentals=0,
        ),
        name="down_product",
    )(numbers, rows, *weights, *pieces)


def flip(value, axis, bit):
    return lax.ppermute(value, axis, [(i, i ^ bit) for i in range(lax.axis_size(axis))])


def silu_sum(first, second):
    pre = first.astype(jnp.float32) + second.astype(jnp.float32)
    return (pre * jax.nn.sigmoid(pre)).astype(jnp.bfloat16)


def plain_sum(first, second):
    return (first.astype(jnp.float32) + second.astype(jnp.float32)).astype(jnp.bfloat16)


def dense_layer(tokens, norm_gain, router, next_router, expert_ids, store, send_list, cache_map):
    tok_dev, width = tokens.shape
    n_ep = lax.axis_size("ep")
    half = n_ep // 2
    experts = router.shape[1]
    tiles = cache_map.shape[1]
    lanes_of = tiles // n_ep
    sub = lanes_of // 2
    tile_rows, tile_cols = store.shape[3:]
    part = width // 2
    row_tiles = part // tile_rows
    col_tiles = tiles // (2 * row_tiles)
    hidden_width = col_tiles * tile_cols
    me, side = lax.axis_index("ep"), lax.axis_index("dp")
    groups = [list(range(half)), list(range(half, n_ep))]
    mirror = ("ep", half)
    beside = ("ep", 1)
    across = ("dp", 1)

    owned = store.reshape(tiles, tile_rows, tile_cols)
    wanted = send_list.reshape(-1)
    place = jnp.reshape(me, (1,)).astype(jnp.int32)

    def near_column(number, i, lane):
        return i * lanes_of + lane

    def far_column(number, j, lane):
        return half * lanes_of + sub * (number ^ j) + lane

    leaving = pick_tiles(near_column, place, wanted, owned, half, lanes_of, True)
    far = pick_tiles(far_column, place, wanted, owned, n_ep, sub, False)

    values = tokens.astype(jnp.float32)
    scale = lax.rsqrt(jnp.mean(values * values, axis=1, keepdims=True) + 1e-06)
    normed = (values * scale * norm_gain).astype(jnp.bfloat16)
    scores = jax.nn.sigmoid(jnp.dot(normed, router, preferred_element_type=jnp.float32))
    chosen = (
        expert_ids[:, :, None] == jnp.arange(experts, dtype=jnp.int32)[None, None, :]
    ).astype(jnp.float32)
    picked = jnp.sum(chosen, axis=1) * scores
    weights = (2.5 * picked / jnp.sum(picked, axis=1, keepdims=True)).astype(jnp.bfloat16)
    digit = tile_cols
    each = -(-tiles // tok_dev)
    codes = jnp.pad(cache_map.reshape(-1), (0, each * tok_dev - tiles)).reshape(tok_dev, each)
    codes = jnp.concatenate([codes // digit, codes % digit], axis=1).astype(jnp.bfloat16)
    used = experts + 2 * each
    lanes = tile_cols * (-(-used // tile_cols))
    first, second = normed[:, :part], normed[:, part:]
    mine = jnp.concatenate(
        [
            jnp.where(side == 0, first, second),
            jnp.pad(jnp.concatenate([weights, codes], axis=1), ((0, 0), (0, lanes - used))),
        ],
        axis=1,
    )
    theirs = jnp.concatenate(
        [
            jnp.where(side == 0, second, first),
            jnp.pad(weights, ((0, 0), (0, lanes - experts))),
        ],
        axis=1,
    )
    rows = jnp.stack([mine, flip(theirs, *across)])
    arrived = lax.all_to_all(
        leaving, "ep", split_axis=0, concat_axis=0, tiled=True, axis_index_groups=groups
    )
    rows = jnp.stack([rows, flip(rows, *mirror)], axis=1)
    blocks = [rows]
    for number in range(2, half, 2):
        blocks.append(flip(rows, "ep", number))
    crossed = [far[0]]
    for j in range(1, n_ep):
        crossed.append(flip(far[j], "ep", j))
    rows = jnp.stack(blocks, axis=2)
    rows = jnp.stack([rows, flip(rows, *beside)], axis=2)
    rows = rows.reshape(2 * n_ep * tok_dev, part + lanes)
    rows, other_router = lax.optimization_barrier((rows, flip(next_router, *across)))

    def map_of(number):
        relative = number ^ me
        block = (relative // half * 2 + relative % 2) * (half // 2) + relative % half // 2
        got = lax.dynamic_slice(
            rows, (block * tok_dev, part + experts), (tok_dev, 2 * each)
        ).astype(jnp.int32)
        return (got[:, :each] * digit + got[:, each:]).reshape(-1)[:tiles]

    expert_of = [me % half, half + me // 2]
    slots = map_of(expert_of[0])
    owner, number = slots // lanes_of, slots % lanes_of
    near = (owner // half) == (me // half)
    map_a = jnp.where(near, owner % half * lanes_of + number, -1)
    slots = map_of(expert_of[1])
    owner, inside = slots // lanes_of, slots % lanes_of - sub * (me % 2)
    map_b = jnp.where((inside >= 0) & (inside < sub), (owner ^ me) * sub + inside, -1)

    def inverse_of(index):
        held = index[None, :] == jnp.arange(tiles // 2, dtype=jnp.int32)[:, None]
        number = jnp.arange(1, tiles + 1, dtype=jnp.int32)[None, :]
        return jnp.sum(jnp.where(held, number, 0), axis=1) - 1

    held_a = (map_a, inverse_of(map_a))
    held_b = (map_b, inverse_of(map_b))
    (map_a, inverse_a), (map_b, inverse_b) = lax.optimization_barrier((held_a, held_b))
    quarter = half * tok_dev
    keep, send = up_product(map_a, inverse_a, rows, [arrived], part, hidden_width, 2 * quarter)
    own = plain_sum(keep, flip(send, *across))
    down_a = place_down(map_a, inverse_a, tiles // 2, [arrived], part, hidden_width)
    own = silu_sum(own[:quarter], flip(own[quarter:], *mirror))
    numbers = jnp.stack(expert_of).astype(jnp.int32)
    whole_router = jnp.where(
        side == 0,
        jnp.concatenate([next_router, other_router], axis=0),
        jnp.concatenate([other_router, next_router], axis=0),
    )
    kept, crossed, down_a, numbers, whole_router = lax.optimization_barrier(
        (own, crossed, down_a, numbers, whole_router)
    )
    swapped = flip(own, *across)
    mirrored = flip(own, *mirror)
    pieces = [kept, mirrored, swapped, flip(swapped, *mirror)]
    layout = [(0, quarter, i * quarter, quarter) for i in range(4)]

    eighth = half // 2 * tok_dev
    keep, send = up_product(map_b, inverse_b, rows, crossed, part, hidden_width, eighth)
    own = plain_sum(keep, flip(send, *beside))
    own = silu_sum(own[:quarter], flip(own[quarter:], *across))
    swapped = flip(own, *across)
    pieces += [own, flip(own, *beside), swapped, flip(swapped, *beside)]
    starts = (0, eighth, 2 * quarter, 2 * quarter + eighth)
    layout += [(1, eighth, start, quarter) for start in starts]
    down_b = place_down(map_b, inverse_b, tiles // 2, crossed, part, hidden_width)

    products = down_product(
        [down_a, down_b],
        pieces,
        layout,
        numbers,
        rows,
        tile_rows * largest_divisor(row_tiles, 7),
        eighth,
    )
    sums = [None, None]
    for d in (1, 0):
        total = plain_sum(products[2 * d], flip(products[2 * d + 1], *beside))
        total = total.reshape(2, half // 2, tok_dev, part)
        pieces = [total[:, 0]]
        for m in range(1, half // 2):
            pieces.append(flip(total[:, m], "ep", 2 * m))
        total = sum(piece.astype(jnp.float32) for piece in pieces).astype(jnp.bfloat16)
        sums[d] = plain_sum(total[0], flip(total[1], *mirror))
    mine, other = sums[0], flip(sums[1], *across)
    mixed = jnp.where(
        side == 0,
        jnp.concatenate([mine, other], axis=1),
        jnp.concatenate([other, mine], axis=1),
    ).astype(jnp.float32)
    layer_out = (values + mixed).astype(jnp.bfloat16)
    stream = layer_out.astype(jnp.float32)
    renorm = lax.rsqrt(jnp.mean(stream * stream, axis=1, keepdims=True) + 1e-06)
    next_normed = (stream * renorm).astype(jnp.bfloat16)
    next_logits = jnp.dot(next_normed, whole_router, preferred_element_type=jnp.float32)
    return (layer_out, jax.nn.sigmoid(next_logits))


def sparse_layer(tokens, norm_gain, router, next_router, expert_ids, store, send_list, cache_map):
    tok_dev, width = tokens.shape
    n_dp = lax.axis_size("dp")
    experts = router.shape[1]
    top = expert_ids.shape[1]
    tiles = cache_map.shape[1]
    tile_rows = store.shape[3]
    tile_cols = store.shape[4]
    part = width // n_dp
    row_tiles = part // tile_rows
    col_tiles = tiles // (2 * row_tiles)
    hidden_width = col_tiles * tile_cols
    capacity = row_capacity(tokens, router, expert_ids)
    values = tokens.astype(jnp.float32)
    scale = lax.rsqrt(jnp.mean(values * values, axis=1, keepdims=True) + 1e-06)
    normed = (values * scale * norm_gain).astype(jnp.bfloat16)
    scores = jax.nn.sigmoid(jnp.dot(normed, router, preferred_element_type=jnp.float32))
    chosen = (expert_ids[:, :, None] == jnp.arange(experts, dtype=jnp.int32)[None, None, :]).astype(
        jnp.float32
    )
    picked = jnp.sum(chosen * scores[:, None, :], axis=2)
    weights = (2.5 * picked / jnp.sum(picked, axis=1, keepdims=True)).astype(jnp.bfloat16)
    flat = chosen.reshape(tok_dev * top, experts)
    before = jnp.cumsum(flat, axis=0) - flat
    rank = jnp.sum(before * flat, axis=1).astype(jnp.int32)
    slot = expert_ids.reshape(-1) * capacity + rank
    columns = jnp.arange(experts * capacity, dtype=jnp.int32)
    match = (slot[:, None] == columns[None, :]).reshape(tok_dev, top, experts * capacity)
    dispatch = jnp.sum(match.astype(jnp.float32), axis=1).astype(jnp.bfloat16)
    combine = jnp.sum(
        jnp.where(match, weights.astype(jnp.float32)[:, :, None], 0.0), axis=1
    ).astype(jnp.bfloat16)
    outgoing = lax.dot_general(
        dispatch, normed, (((0,), (0,)), ((), ())), preferred_element_type=jnp.float32
    ).astype(jnp.bfloat16)
    owned = store.reshape(store.shape[2], tile_rows, tile_cols)
    leaving = owned[jnp.maximum(send_list.reshape(-1), 0)]
    arrived = lax.all_to_all(leaving, "ep", split_axis=0, concat_axis=0, tiled=True)
    cached = arrived[cache_map.reshape(-1)].reshape(2, row_tiles, col_tiles, tile_rows, tile_cols)
    up_tiles = cached[0]
    down_tiles = cached[1]
    rows = lax.all_to_all(
        lax.all_to_all(outgoing, "ep", split_axis=0, concat_axis=0, tiled=True),
        "dp",
        split_axis=1,
        concat_axis=0,
        tiled=True,
    )
    count = rows.shape[0]
    block = rows.reshape(count, row_tiles, tile_rows)
    product = jnp.einsum("nat,acts->ncs", block, up_tiles, preferred_element_type=jnp.float32)
    summed = lax.psum(product.reshape(count, hidden_width).astype(jnp.bfloat16), "dp").astype(
        jnp.float32
    )
    hidden = jax.nn.silu(summed).astype(jnp.bfloat16)
    number = hidden.shape[0]
    product = jnp.einsum(
        "ncs,acts->nat",
        hidden.reshape(number, col_tiles, tile_cols),
        down_tiles,
        preferred_element_type=jnp.float32,
    )
    result = product.reshape(number, part).astype(jnp.bfloat16)
    back = lax.all_to_all(
        lax.all_to_all(result, "dp", split_axis=0, concat_axis=1, tiled=True),
        "ep",
        split_axis=0,
        concat_axis=0,
        tiled=True,
    )
    mixed = jnp.dot(combine, back, preferred_element_type=jnp.float32)
    layer_out = (values + mixed).astype(jnp.bfloat16)
    stream = layer_out.astype(jnp.float32)
    renorm = lax.rsqrt(jnp.mean(stream * stream, axis=1, keepdims=True) + 1e-06)
    next_normed = (stream * renorm).astype(jnp.bfloat16)
    features = lax.all_to_all(next_normed, "dp", split_axis=1, concat_axis=0, tiled=True)
    partial_scores = jnp.dot(features, next_router, preferred_element_type=jnp.float32)
    next_logits = lax.psum_scatter(
        partial_scores.astype(jnp.bfloat16), "dp", scatter_dimension=0, tiled=True
    ).astype(jnp.float32)
    return (layer_out, jax.nn.sigmoid(next_logits))


def row_capacity(tokens, router, expert_ids):
    tok_dev, experts, top = tokens.shape[0], router.shape[1], expert_ids.shape[1]
    return min(tok_dev, max(2, 2 * tok_dev * top // experts))


def per_device(*arrays):
    tokens, _, router, _, expert_ids, store, send_list, cache_map = arrays
    n_ep = lax.axis_size("ep")
    every_row = row_capacity(tokens, router, expert_ids) == tokens.shape[0]
    one_each = router.shape[1] == n_ep and store.shape[2] == cache_map.shape[1]
    two_power = n_ep > 2 and n_ep & (n_ep - 1) == 0
    one_each = one_each and send_list.shape[1] == cache_map.shape[1]
    one_each = one_each and cache_map.shape[1] % (2 * n_ep) == 0
    if every_row and one_each and two_power and lax.axis_size("dp") == 2:
        return dense_layer(*arrays)
    return sparse_layer(*arrays)


def solution(mesh):
    in_specs = (
        P(("ep", "dp"), None),
        P(),
        P(),
        P("dp", None),
        P(("ep", "dp"), None),
        P("ep", "dp", None, None, None),
        P("ep", None),
        P("ep", None),
    )
    out_specs = (P(("ep", "dp"), None), P(("ep", "dp"), None))
    return jax.shard_map(
        per_device, mesh=mesh, in_specs=in_specs, out_specs=out_specs, check_vma=False
    )
```
